16 devices in a mesh: depth: 2 (over z), col: 2 (over y), row: 4 (over x, core).
Axes of the slice: x: 2, y: 2, z: 2, core: 2. Of those that a mesh axis runs over, the one named last changes fastest.
Arguments:
- tokens: bfloat16 [32768, 1280], P(('depth', 'row'), 'col')
- w_up: bfloat16 [1280, 5120], P('row', 'col')
- w_down: bfloat16 [5120, 1280], P('row', 'col')
- grad_out: bfloat16 [32768, 1280], P(('depth', 'row'), 'col')
Outputs:
- output 1: bfloat16 [32768, 1280], P(('depth', 'row'), 'col')
- output 2: bfloat16 [32768, 1280], P(('depth', 'row'), 'col')
- output 3: float32 [1280, 5120], P('row', 'col')
- output 4: float32 [5120, 1280], P('row', 'col')
All inputs are finite; a program needn't handle non-finite values.
Results may differ from the reference program's by a relative error of at most 0.001.
Values are sent between devices in bfloat16 or wider.
A program may use at most 1 GiB of HBM per device.

```python
import jax
import jax.numpy as jnp
from jax import lax

H = 1280
F = 5120
ROWS = 4096
SHARDS = 8
TOKENS = ROWS * SHARDS


def gelu_fn(pre_act):
    return jax.nn.gelu(pre_act, approximate=True)


def setup_inputs(seed: int = 0) -> dict:
    root_key = jax.random.key(seed)
    key_tok, key_up, key_down, key_grad = jax.random.split(root_key, 4)
    tokens = jax.random.normal(key_tok, (TOKENS, H), jnp.float32)
    w_up = jax.random.normal(key_up, (H, F), jnp.float32) * H ** -0.5
    w_down = jax.random.normal(key_down, (F, H), jnp.float32) * F ** -0.5
    grad_out = jax.random.normal(key_grad, (TOKENS, H), jnp.float32)
    return {"tokens": tokens.astype(jnp.bfloat16), "w_up": w_up.astype(jnp.bfloat16), "w_down": w_down.astype(jnp.bfloat16), "grad_out": grad_out.astype(jnp.bfloat16)}


def reference(tokens, w_up, w_down, grad_out):
    tok_blocks = tokens.reshape(SHARDS, ROWS, H)
    grad_blocks = grad_out.reshape(SHARDS, ROWS, H)

    def shard_step(acc_pair, blocks):
        acc_up, acc_down = acc_pair
        tok_blk, grad_blk = blocks
        pre_act = jnp.dot(tok_blk, w_up, preferred_element_type=jnp.float32)
        hidden, gelu_vjp = jax.vjp(gelu_fn, pre_act)
        hidden = hidden.astype(jnp.bfloat16)
        out_blk = jnp.dot(hidden, w_down, preferred_element_type=jnp.float32).astype(jnp.bfloat16)
        d_hidden = jnp.dot(grad_blk, w_down.T, preferred_element_type=jnp.float32)
        d_pre = gelu_vjp(d_hidden)[0].astype(jnp.bfloat16)
        dx_blk = jnp.dot(d_pre, w_up.T, preferred_element_type=jnp.float32).astype(jnp.bfloat16)
        acc_up = acc_up + jnp.dot(tok_blk.T, d_pre, preferred_element_type=jnp.float32)
        acc_down = acc_down + jnp.dot(hidden.T, grad_blk, preferred_element_type=jnp.float32)
        return (acc_up, acc_down), (out_blk, dx_blk)

    init_pair = (jnp.zeros((H, F), jnp.float32), jnp.zeros((F, H), jnp.float32))
    (dw_up, dw_down), (out_blocks, dx_blocks) = lax.scan(shard_step, init_pair, (tok_blocks, grad_blocks))
    return out_blocks.reshape(TOKENS, H), dx_blocks.reshape(TOKENS, H), dw_up, dw_down
```

```python
import jax
import jax.numpy as jnp
from jax import lax
from jax.experimental import pallas as pl
from jax.experimental.pallas import tpu as pltpu
from jax.sharding import PartitionSpec as P


BF16, F32 = jnp.bfloat16, jnp.float32
VMEM_LIMIT = 60 * 1024 * 1024
SQRT_2_OVER_PI = 0.7978845608028654
CUBIC = 0.044715
NCHUNK = 4
NPIECE = 4
LAST_LAST = (((1,), (1,)), ((), ()))


def dot(a, b):
    return jnp.dot(a, b, preferred_element_type=F32)


def dot_t(a, b):
    return lax.dot_general(a, b, LAST_LAST, preferred_element_type=F32)


def cost(flops, nbytes, trans=0):
    return pl.CostEstimate(flops=flops, bytes_accessed=nbytes, transcendentals=trans)


def params():
    return pltpu.CompilerParams(vmem_limit_bytes=VMEM_LIMIT)


def up_body(s_ref, xo_ref, xt_ref, wo_ref, wt_ref, *rest):
    a_ref, d_ref = rest[-2:]
    rows = xo_ref.shape[0]
    sub = 256
    for i in range(rows // sub):
        sl = pl.ds(i * sub, sub)
        u = dot(xo_ref[sl, :], wo_ref[...]) + dot(xt_ref[sl, :], wt_ref[...])
        u2 = u * u
        t = jnp.tanh(u * (SQRT_2_OVER_PI + (SQRT_2_OVER_PI * CUBIC) * u2))
        h = 0.5 + 0.5 * t
        a_ref[sl, :] = (u * h).astype(BF16)
        slope = SQRT_2_OVER_PI + (3.0 * SQRT_2_OVER_PI * CUBIC) * u2
        d_ref[sl, :] = h + ((1.0 - t * t) * (0.5 * u)) * slope


def up_kernel(s, x_own, x_oth, w1, chunk, bufs, bn=512):
    tokens, hh = x_own.shape
    rows = x_oth.shape[0]
    f = w1.shape[1]
    in_specs = [
        pl.BlockSpec((rows, hh), lambda j, s: (chunk, 0)),
        pl.BlockSpec((rows, hh), lambda j, s: (0, 0)),
        pl.BlockSpec((hh, bn), lambda j, s: (s[0], j)),
        pl.BlockSpec((hh, bn), lambda j, s: (1 - s[0], j)),
    ]
    out_spec = pl.BlockSpec((rows, bn), lambda j, s: (chunk, j))
    args = [s, x_own, x_oth, w1, w1]
    aliases = {}
    if bufs is not None:
        in_specs += [pl.BlockSpec(memory_space=pl.ANY)] * 2
        args += list(bufs)
        aliases = {5: 0, 6: 1}
    return pl.pallas_call(
        up_body,
        grid_spec=pltpu.PrefetchScalarGridSpec(
            num_scalar_prefetch=1, grid=(f // bn,), in_specs=in_specs, out_specs=[out_spec, out_spec]),
        out_shape=[jax.ShapeDtypeStruct((tokens, f), BF16), jax.ShapeDtypeStruct((tokens, f), F32)],
        input_output_aliases=aliases,
        compiler_params=params(),
        cost_estimate=cost(2 * rows * 2 * hh * f, rows * f * 6 + 2 * hh * f * 2, rows * f),
        name="up",
    )(*args)


def du_body(go_ref, gt_ref, wo_ref, wt_ref, d_ref, *rest):
    u_ref = rest[-1]
    rows = go_ref.shape[0]
    sub = 256
    for i in range(rows // sub):
        sl = pl.ds(i * sub, sub)
        da = dot_t(go_ref[sl, :], wo_ref[...]) + dot_t(gt_ref[sl, :], wt_ref[...])
        u_ref[sl, :] = (da * d_ref[sl, :]).astype(BF16)


def du_kernel(g_own, g_oth, w2_own, w2_oth, d, chunk, buf, bn=512):
    tokens, hh = g_own.shape
    rows = g_oth.shape[0]
    f = w2_own.shape[0]
    in_specs = [
        pl.BlockSpec((rows, hh), lambda j: (chunk, 0)),
        pl.BlockSpec((rows, hh), lambda j: (0, 0)),
        pl.BlockSpec((bn, hh), lambda j: (j, 0)),
        pl.BlockSpec((bn, hh), lambda j: (j, 0)),
        pl.BlockSpec((rows, bn), lambda j: (chunk, j)),
    ]
    args = [g_own, g_oth, w2_own, w2_oth, d]
    aliases = {}
    if buf is not None:
        in_specs.append(pl.BlockSpec(memory_space=pl.ANY))
        args.append(buf)
        aliases = {5: 0}
    return pl.pallas_call(
        du_body,
        grid=(f // bn,),
        in_specs=in_specs,
        out_specs=pl.BlockSpec((rows, bn), lambda j: (chunk, j)),
        out_shape=jax.ShapeDtypeStruct((tokens, f), BF16),
        input_output_aliases=aliases,
        compiler_params=params(),
        cost_estimate=cost(2 * rows * 2 * hh * f, rows * f * 6 + 2 * hh * f * 2),
        name="du",
    )(*args)


def y_body(a_ref, w_ref, o_ref):
    o_ref[...] = dot(a_ref[...], w_ref[...]).astype(BF16)


def y_kernel(a, w2_own, bm=512):
    tokens, f = a.shape
    n = w2_own.shape[1]
    return pl.pallas_call(
        y_body,
        grid=(tokens // bm,),
        in_specs=[pl.BlockSpec((bm, f), lambda i: (i, 0)), pl.BlockSpec((f, n), lambda i: (0, 0))],
        out_specs=pl.BlockSpec((bm, n), lambda i: (i, 0)),
        out_shape=jax.ShapeDtypeStruct((tokens, n), BF16),
        compiler_params=params(),
        cost_estimate=cost(2 * tokens * f * n, tokens * f * 2 + f * n * 2),
        name="y",
    )(a, w2_own)


def dx_body(s_ref, u_ref, w_ref, o_ref):
    o_ref[...] = dot_t(u_ref[...], w_ref[...]).astype(BF16)


def dx_kernel(s, du, w1, hh, bm=512):
    tokens, f = du.shape
    return pl.pallas_call(
        dx_body,
        grid_spec=pltpu.PrefetchScalarGridSpec(
            num_scalar_prefetch=1,
            grid=(tokens // bm,),
            in_specs=[
                pl.BlockSpec((bm, f), lambda i, s: (i, 0)),
                pl.BlockSpec((hh, f), lambda i, s: (s[0], 0)),
            ],
            out_specs=pl.BlockSpec((bm, hh), lambda i, s: (i, 0))),
        out_shape=jax.ShapeDtypeStruct((tokens, hh), BF16),
        compiler_params=params(),
        cost_estimate=cost(2 * tokens * f * hh, tokens * f * 2 + f * hh * 2),
        name="dx",
    )(s, du, w1)


def dw2_body(s_ref, g_ref, a_ref, o_ref):
    o_ref[...] = dot(g_ref[...], a_ref[...])


def dw2_kernel(idx, g_t, a, width, bn=256):
    n, tokens = g_t.shape
    steps = width // bn
    return pl.pallas_call(
        dw2_body,
        grid_spec=pltpu.PrefetchScalarGridSpec(
            num_scalar_prefetch=1,
            grid=(steps,),
            in_specs=[
                pl.BlockSpec((n, tokens), lambda j, s: (0, 0)),
                pl.BlockSpec((tokens, bn), lambda j, s: (0, s[0] * steps + j)),
            ],
            out_specs=pl.BlockSpec((n, bn), lambda j, s: (0, j))),
        out_shape=jax.ShapeDtypeStruct((n, width), F32),
        compiler_params=params(),
        cost_estimate=cost(2 * tokens * n * width, tokens * (n + width) * 2 + n * width * 4),
        name="dw2",
    )(idx, g_t, a)


def dw1_body(s_ref, x_ref, u_ref, mine_ref, theirs_ref):
    r = dot(x_ref[...], u_ref[...])
    half = r.shape[0] // 2

    @pl.when(s_ref[2] == 0)
    def _():
        mine_ref[...] = r[:half]
        theirs_ref[...] = r[half:]

    @pl.when(s_ref[2] != 0)
    def _():
        mine_ref[...] = r[half:]
        theirs_ref[...] = r[:half]


def dw1_kernel(s, x_t, du, width, part, nparts, bn=256):
    hrows, tokens = x_t.shape
    half = hrows // 2
    steps = width // nparts // bn
    out_spec = pl.BlockSpec((half // 2, bn), lambda j, s: (0, j))
    shape = jax.ShapeDtypeStruct((half // 2, width // nparts), F32)
    return pl.pallas_call(
        dw1_body,
        grid_spec=pltpu.PrefetchScalarGridSpec(
            num_scalar_prefetch=1,
            grid=(steps,),
            in_specs=[
                pl.BlockSpec((half, tokens), lambda j, s: (s[0], 0)),
                pl.BlockSpec((tokens, bn), lambda j, s: (0, (s[1] * nparts + part) * steps + j)),
            ],
            out_specs=[out_spec, out_spec]),
        out_shape=[shape, shape],
        compiler_params=params(),
        cost_estimate=cost(2 * tokens * half * width // nparts, tokens * (half + width // nparts) * 2 + half * width * 4 // nparts),
        name="dw1",
    )(s, x_t, du)


def solution(mesh):
    nx = mesh.shape["row"] // 2
    act_spec = P(("depth", "row"), "col")
    weight_spec = P("row", "col")
    pair = [(0, 1), (1, 0)]
    core_pair = [(r, r ^ 1) for r in range(2 * nx)]
    x_pair = [(r, r ^ 2) for r in range(2 * nx)]

    def over_core(v):
        return lax.ppermute(v, "row", core_pair)

    def over_x(v):
        return lax.ppermute(v, "row", x_pair)

    def over_col(v):
        return lax.ppermute(v, "col", pair)

    def over_depth(v):
        return lax.ppermute(v, "depth", pair)

    def body(tok, up, down, grad):
        col = lax.axis_index("col")
        row = lax.axis_index("row")
        depth = lax.axis_index("depth")
        x, core = row // 2, row % 2
        tokens, hh = tok.shape
        rows = tokens // NCHUNK
        fh = up.shape[1]

        def half_block(blk):
            n = blk.shape[0] // 2
            return lax.dynamic_slice_in_dim(blk, depth * n, n, 0)

        def other_block(blk):
            first = over_col(half_block(blk))
            second = over_depth(first)
            lo = jnp.where(depth == 0, first, second)
            hi = jnp.where(depth == 0, second, first)
            return jnp.concatenate([lo, hi], axis=0)

        def row_blocks(blk):
            b_c = over_core(blk)
            b_x = over_x(blk)
            b_xc = over_core(b_x)
            return ((row, blk), (row ^ 1, b_c), (row ^ 2, b_x), (row ^ 3, b_xc))

        up_oth = other_block(up)
        tok_oth = []
        grad_oth = []
        for i in range(NCHUNK):
            tok_oth.append(over_col(tok[i * rows:(i + 1) * rows]))
        down_oth = other_block(down)
        for i in range(NCHUNK):
            grad_oth.append(over_col(grad[i * rows:(i + 1) * rows]))

        w1 = jnp.zeros((4 * up.shape[0], 2 * fh), BF16)
        for r, b in row_blocks(up):
            w1 = lax.dynamic_update_slice(w1, b, (r * up.shape[0], col * fh))
        for r, b in row_blocks(up_oth):
            w1 = lax.dynamic_update_slice(w1, b, (r * up.shape[0], (1 - col) * fh))
        w2_own = jnp.zeros((4 * down.shape[0], hh), BF16)
        for r, b in row_blocks(down):
            w2_own = lax.dynamic_update_slice(w2_own, b, (r * down.shape[0], 0))
        w2_oth = jnp.zeros((4 * down.shape[0], hh), BF16)
        for r, b in row_blocks(down_oth):
            w2_oth = lax.dynamic_update_slice(w2_oth, b, (r * down.shape[0], 0))

        grad_t = grad.T
        x_t = jnp.zeros((2 * hh, tokens), BF16)
        x_t = lax.dynamic_update_slice(x_t, tok.T, (col * hh, 0))
        for i in range(NCHUNK):
            x_t = lax.dynamic_update_slice(x_t, tok_oth[i].T, ((1 - col) * hh, i * rows))

        scol = jnp.stack([col])
        bufs = None
        for i in range(NCHUNK):
            bufs = up_kernel(scol, tok, tok_oth[i], w1, i, bufs)
        a, d = bufs

        fb = down.shape[0]
        parts = {}
        for q in (3, 2, 1, 0):
            parts[q] = dw2_kernel(jnp.stack([row ^ q]), grad_t, a, fb)
        got3 = over_core(parts[3])
        got1 = over_core(parts[1])
        n = hh // NPIECE
        pieces = []
        for p in range(NPIECE):
            sl = slice(p * n, (p + 1) * n)
            away = parts[2][sl] + got3[sl]
            came = over_x(away)
            layer = (parts[0][sl] + got1[sl]) + came
            pieces.append((layer + over_depth(layer)).T)
        dw_down = jnp.concatenate(pieces, axis=1)

        du = None
        for i in range(NCHUNK):
            du = du_kernel(grad, grad_oth[i], w2_own, w2_oth, d, i, du)

        nparts = 2
        s_away = jnp.stack([1 - x, col, core])
        s_here = jnp.stack([x, col, core])
        away = [dw1_kernel(s_away, x_t, du, fh, p, nparts) for p in range(nparts)]
        here = [dw1_kernel(s_here, x_t, du, fh, p, nparts) for p in range(nparts)]
        cols = []
        per = NPIECE // nparts
        for p in range(nparts):
            got_away = over_core(away[p][1])
            got_here = over_core(here[p][1])
            w = fh // NPIECE
            for q in range(per):
                sl = slice(q * w, (q + 1) * w)
                out = away[p][0][:, sl] + got_away[:, sl]
                came = over_x(out)
                layer = (here[p][0][:, sl] + got_here[:, sl]) + came
                cols.append(layer + over_depth(layer))
        dw_up = jnp.concatenate(cols, axis=1)

        out_blk = y_kernel(a, w2_own)
        dx_blk = dx_kernel(scol, du, w1, hh)
        return out_blk, dx_blk, dw_up, dw_down

    return jax.shard_map(body, mesh=mesh, in_specs=(act_spec, weight_spec, weight_spec, act_spec),
                         out_specs=(act_spec, act_spec, weight_spec, weight_spec), check_vma=False)
```

```python
import jax
import jax.numpy as jnp
from jax import lax
from jax.experimental import pallas as pl
from jax.experimental.pallas import tpu as pltpu
from jax.sharding import PartitionSpec as P


BF16, F32 = jnp.bfloat16, jnp.float32
VMEM_LIMIT = 60 * 1024 * 1024
SQRT_2_OVER_PI = 0.7978845608028654
CUBIC = 0.044715
NCHUNK = 4
NFIRST = 2
NPIECE2 = 2
NPIECE1 = 4
NOUT = 2
SUB = 512
MESH = pl.DeviceIdType.MESH
LAST_LAST = (((1,), (1,)), ((), ()))


def dot(a, b):
    return jnp.dot(a, b, preferred_element_type=F32)


def dot_t(a, b):
    return lax.dot_general(a, b, LAST_LAST, preferred_element_type=F32)


def cost(flops, nbytes, trans=0):
    return pl.CostEstimate(flops=flops, bytes_accessed=nbytes, transcendentals=trans)


def params():
    return pltpu.CompilerParams(vmem_limit_bytes=VMEM_LIMIT)


def gather_body(w1_ref, w2_ref, tok_ref, w1, w2, tok_oth, send, recv, local):
    col, row, depth = lax.axis_index("col"), lax.axis_index("row"), lax.axis_index("depth")
    x, core = row // 2, row % 2
    to_core = {"row": 2 * x + (1 - core)}
    to_x = {"row": 2 * (1 - x) + core}
    to_col = {"col": 1 - col}
    to_depth = {"depth": 1 - depth}

    barrier = pltpu.get_barrier_semaphore()
    for dev in (to_core, to_x, to_col, to_depth):
        pl.semaphore_signal(barrier, inc=1, device_id=dev, device_id_type=MESH)
    pl.semaphore_wait(barrier, 4)

    def place(which, bx, bcol, at_col, half=None):
        ref = (w1_ref, w2_ref)[which]
        n, m = ref.shape
        side = (bx + at_col) % 2 if which == 0 else (bcol + at_col) % 2
        if which == 0:
            r0, c0 = side * (2 * n) + core * n, bcol * m
        else:
            r0, c0 = (2 * bx + core) * n, side * m
        if half is not None:
            r0, n = r0 + half * (n // 2), n // 2
        return (w1, w2)[which].at[pl.ds(pl.multiple_of(r0, 32), n), pl.ds(pl.multiple_of(c0, 128), m)]

    made = []

    def start(src, dst, dev):
        i = len(made)
        cp = pltpu.make_async_remote_copy(src_ref=src, dst_ref=dst, send_sem=send.at[i], recv_sem=recv.at[i],
                                          device_id=dev, device_id_type=MESH)
        cp.start()
        made.append(cp)
        return cp

    def forward(piece, dev):
        return start(piece, piece, dev)

    def half_of(ref):
        n = ref.shape[0] // 2
        return ref.at[pl.ds(pl.multiple_of(depth * n, 32), n), :]

    late = []

    def to_partner(piece):
        late.append(forward(piece, to_core))

    other = 1 - col
    col1 = start(half_of(w1_ref), place(0, x, col, other, depth), to_col)
    x1 = start(w1_ref, place(0, x, col, col), to_x)
    col2 = start(half_of(w2_ref), place(1, x, col, other, depth), to_col)
    first = tok_oth.shape[0]
    late.append(start(tok_ref.at[pl.ds(0, first), :], tok_oth, to_col))
    late.append(start(w1_ref, place(0, x, col, col), to_core))
    late.append(start(w2_ref, place(1, x, col, col), to_core))
    keep = [pltpu.make_async_copy(w1_ref, place(0, x, col, col), local.at[0]),
            pltpu.make_async_copy(w2_ref, place(1, x, col, col), local.at[1])]
    for cp in keep:
        cp.start()

    def oth(which, bx, half):
        return place(which, bx, other, col, half)

    col1.wait_recv()
    z1 = forward(oth(0, x, depth), to_depth)
    x1h = forward(oth(0, x, depth), to_x)
    to_partner(oth(0, x, depth))
    x2 = start(half_of(w2_ref), place(1, x, col, col, depth), to_x)
    col2.wait_recv()
    z2 = forward(oth(1, x, depth), to_depth)
    x2h = forward(oth(1, x, depth), to_x)
    to_partner(oth(1, x, depth))
    z1.wait_recv()
    to_partner(oth(0, x, 1 - depth))
    x1.wait_recv()
    to_partner(place(0, 1 - x, col, col))
    x1h.wait_recv()
    z1d = forward(oth(0, 1 - x, depth), to_depth)
    to_partner(oth(0, 1 - x, depth))
    z2.wait_recv()
    to_partner(oth(1, x, 1 - depth))
    x2.wait_recv()
    z2o = forward(place(1, 1 - x, col, col, depth), to_depth)
    to_partner(place(1, 1 - x, col, col, depth))
    z1d.wait_recv()
    to_partner(oth(0, 1 - x, 1 - depth))
    x2h.wait_recv()
    z2d = forward(oth(1, 1 - x, depth), to_depth)
    to_partner(oth(1, 1 - x, depth))
    z2o.wait_recv()
    to_partner(place(1, 1 - x, col, col, 1 - depth))
    z2d.wait_recv()
    to_partner(oth(1, 1 - x, 1 - depth))
    for cp in late:
        cp.wait_recv()
    for cp in made:
        cp.wait_send()
    for cp in keep:
        cp.wait()


NCOPY = 25


def gather_kernel(up, down, tok, first):
    return pl.pallas_call(
        gather_body,
        in_specs=[pl.BlockSpec(memory_space=pl.ANY)] * 3,
        out_specs=[pl.BlockSpec(memory_space=pl.ANY)] * 3,
        out_shape=[jax.ShapeDtypeStruct((4 * up.shape[0], 2 * up.shape[1]), BF16),
                   jax.ShapeDtypeStruct((4 * down.shape[0], 2 * down.shape[1]), BF16),
                   jax.ShapeDtypeStruct((first, tok.shape[1]), BF16)],
        scratch_shapes=[pltpu.SemaphoreType.DMA((NCOPY,)), pltpu.SemaphoreType.DMA((NCOPY,)), pltpu.SemaphoreType.DMA((2,))],
        compiler_params=pltpu.CompilerParams(collective_id=0, has_side_effects=True),
        cost_estimate=cost(0, 300_000_000),
        name="gather",
    )(up, down, tok)


ANY = pl.BlockSpec(memory_space=pl.ANY)


def up_body(xo_ref, xt_ref, w_ref, *rest):
    a_ref, d_ref, x_ref = rest[-3:]
    hh = xo_ref.shape[1]

    @pl.when(pl.program_id(0) == 0)
    def _():
        x_ref[:, :hh] = xo_ref[...]
        x_ref[:, hh:] = xt_ref[...]

    rows = xo_ref.shape[0]
    for i in range(rows // SUB):
        sl = pl.ds(i * SUB, SUB)
        u = dot(x_ref[sl, :], w_ref[...])
        u2 = u * u
        t = jnp.tanh(u * (SQRT_2_OVER_PI + (SQRT_2_OVER_PI * CUBIC) * u2))
        h = 0.5 + 0.5 * t
        a_ref[sl, :] = (u * h).astype(BF16)
        slope = SQRT_2_OVER_PI + (3.0 * SQRT_2_OVER_PI * CUBIC) * u2
        d_ref[sl, :] = h + ((1.0 - t * t) * (0.5 * u)) * slope


def up_kernel(x_own, x_oth, at, w1, rows, chunk, bufs, bn=512):
    tokens, hh = x_own.shape
    f = w1.shape[1]
    in_specs = [
        pl.BlockSpec((rows, hh), lambda j: (chunk, 0)),
        pl.BlockSpec((rows, hh), lambda j: (at, 0)),
        pl.BlockSpec((2 * hh, bn), lambda j: (0, j)),
    ]
    out_spec = pl.BlockSpec((rows, bn), lambda j: (chunk, j))
    args = [x_own, x_oth, w1]
    aliases = {}
    if bufs is not None:
        in_specs += [ANY] * 2
        args += list(bufs)
        aliases = {3: 0, 4: 1}
    return pl.pallas_call(
        up_body,
        grid=(f // bn,),
        in_specs=in_specs,
        out_specs=[out_spec, out_spec],
        scratch_shapes=[pltpu.VMEM((rows, 2 * hh), BF16)],
        out_shape=[jax.ShapeDtypeStruct((tokens, f), BF16), jax.ShapeDtypeStruct((tokens, f), F32)],
        input_output_aliases=aliases,
        compiler_params=params(),
        cost_estimate=cost(2 * rows * 2 * hh * f, rows * f * 6 + 2 * hh * f * 2, rows * f),
        name="up",
    )(*args)


def du_body(go_ref, gt_ref, w_ref, d_ref, *rest):
    u_ref, g_ref = rest[-2:]
    hh = go_ref.shape[1]

    @pl.when(pl.program_id(0) == 0)
    def _():
        g_ref[:, :hh] = go_ref[...]
        g_ref[:, hh:] = gt_ref[...]

    rows = go_ref.shape[0]
    for i in range(rows // SUB):
        sl = pl.ds(i * SUB, SUB)
        u_ref[sl, :] = (dot_t(g_ref[sl, :], w_ref[...]) * d_ref[sl, :]).astype(BF16)


def du_kernel(g_own, g_oth, at, w2, d, rows, chunk, buf, after, bn=512):
    tokens, hh = g_own.shape
    f = w2.shape[0]
    in_specs = [
        pl.BlockSpec((rows, hh), lambda j: (chunk, 0)),
        pl.BlockSpec((rows, hh), lambda j: (at, 0)),
        pl.BlockSpec((bn, 2 * hh), lambda j: (j, 0)),
        pl.BlockSpec((rows, bn), lambda j: (chunk, j)),
        ANY,
    ]
    args = [g_own, g_oth, w2, d, after if buf is None else buf]
    return pl.pallas_call(
        du_body,
        grid=(f // bn,),
        in_specs=in_specs,
        out_specs=pl.BlockSpec((rows, bn), lambda j: (chunk, j)),
        scratch_shapes=[pltpu.VMEM((rows, 2 * hh), BF16)],
        out_shape=jax.ShapeDtypeStruct((tokens, f), BF16),
        input_output_aliases={} if buf is None else {4: 0},
        compiler_params=params(),
        cost_estimate=cost(2 * rows * 2 * hh * f, rows * f * 6 + 2 * hh * f * 2),
        name="du",
    )(*args)


def y_body(a_ref, w_ref, dep_ref, o_ref):
    o_ref[...] = dot(a_ref[...], w_ref[...]).astype(BF16)


def dx_body(u_ref, w_ref, dep_ref, o_ref):
    o_ref[...] = dot_t(u_ref[...], w_ref[...]).astype(BF16)


def out_kernel(body, a, w, w_shape, hh, part, nparts, after, chained, bm=512):
    tokens, f = a.shape
    steps = tokens // nparts // bm
    return pl.pallas_call(
        body,
        grid=(steps,),
        in_specs=[pl.BlockSpec((bm, f), lambda i: (part * steps + i, 0)), pl.BlockSpec(w_shape, lambda i: (0, 0)), ANY],
        out_specs=pl.BlockSpec((bm, hh), lambda i: (part * steps + i, 0)),
        out_shape=jax.ShapeDtypeStruct((tokens, hh), BF16),
        input_output_aliases={2: 0} if chained else {},
        compiler_params=params(),
        cost_estimate=cost(2 * tokens * f * hh // nparts, tokens * f * 2 // nparts + f * hh * 2),
    )(a, w, after)


def dw2_body(s_ref, g_ref, a_ref, dep_ref, o_ref):
    o_ref[...] = dot(g_ref[...], a_ref[...])


def dw2_kernel(idx, g_t, a, width, after, bn=512):
    n, tokens = g_t.shape
    steps = width // bn
    return pl.pallas_call(
        dw2_body,
        grid_spec=pltpu.PrefetchScalarGridSpec(
            num_scalar_prefetch=1,
            grid=(steps,),
            in_specs=[
                pl.BlockSpec((n, tokens), lambda j, s: (0, 0)),
                pl.BlockSpec((tokens, bn), lambda j, s: (0, s[0] * steps + j)),
                ANY,
            ],
            out_specs=pl.BlockSpec((n, bn), lambda j, s: (0, j))),
        out_shape=jax.ShapeDtypeStruct((n, width), F32),
        compiler_params=params(),
        cost_estimate=cost(2 * tokens * n * width, tokens * (n + width) * 2 + n * width * 4),
        name="dw2",
    )(idx, g_t, a, after)


def dw1_body(s_ref, x_ref, u_ref, dep_ref, mine_ref, theirs_ref):
    r = dot(x_ref[...], u_ref[...])
    half = r.shape[0] // 2

    @pl.when(s_ref[2] == 0)
    def _():
        mine_ref[...] = r[:half]
        theirs_ref[...] = r[half:]

    @pl.when(s_ref[2] != 0)
    def _():
        mine_ref[...] = r[half:]
        theirs_ref[...] = r[:half]


def dw1_kernel(s, x_t, du, width, after, bn=512):
    hrows, tokens = x_t.shape
    half = hrows // 2
    steps = width // bn
    out_spec = pl.BlockSpec((half // 2, bn), lambda j, s: (0, j))
    shape = jax.ShapeDtypeStruct((half // 2, width), F32)
    return pl.pallas_call(
        dw1_body,
        grid_spec=pltpu.PrefetchScalarGridSpec(
            num_scalar_prefetch=1,
            grid=(steps,),
            in_specs=[
                pl.BlockSpec((half, tokens), lambda j, s: (s[0], 0)),
                pl.BlockSpec((tokens, bn), lambda j, s: (0, s[1] * steps + j)),
                ANY,
            ],
            out_specs=[out_spec, out_spec]),
        out_shape=[shape, shape],
        compiler_params=params(),
        cost_estimate=cost(2 * tokens * half * width, tokens * (half + width) * 2 + half * width * 4),
        name="dw1",
    )(s, x_t, du, after)


def solution(mesh):
    nx = mesh.shape["row"] // 2
    act_spec = P(("depth", "row"), "col")
    weight_spec = P("row", "col")
    pair = [(0, 1), (1, 0)]
    core_pair = [(r, r ^ 1) for r in range(2 * nx)]
    x_pair = [(r, r ^ 2) for r in range(2 * nx)]

    def over_core(v):
        return lax.ppermute(v, "row", core_pair)

    def over_x(v):
        return lax.ppermute(v, "row", x_pair)

    def over_col(v):
        return lax.ppermute(v, "col", pair)

    def over_depth(v):
        return lax.ppermute(v, "depth", pair)

    def body(tok, up, down, grad):
        col = lax.axis_index("col")
        row = lax.axis_index("row")
        x, core = row // 2, row % 2
        tokens, hh = tok.shape
        rows = tokens // NCHUNK
        fh = up.shape[1]

        w1, w2, tok_first = gather_kernel(up, down, tok, NFIRST * rows)
        tok_oth = [(tok_first, i) for i in range(NFIRST)]
        for i in range(NFIRST, NCHUNK):
            tok_oth.append((over_col(tok[i * rows:(i + 1) * rows]), 0))
        grad_oth = [(over_col(grad[i * rows:(i + 1) * rows]), 0) for i in range(NCHUNK)]

        grad_t = grad.T
        x_t = jnp.concatenate([tok.T, jnp.concatenate([tok_first.T] + [t.T for t, _ in tok_oth[NFIRST:]], axis=1)], axis=0)

        bufs = None
        for i in range(NCHUNK):
            bufs = up_kernel(tok, *tok_oth[i], w1, rows, i, bufs)
        a, d = bufs

        away = dw2_kernel(jnp.stack([1 - x]), grad_t, a, fh, d)
        here = dw2_kernel(jnp.stack([x]), grad_t, a, fh, away)
        fb = fh // 2

        def of_core(v, c, r0, n):
            return lax.dynamic_slice(v, (r0, c * fb), (n, fb))

        got_away = over_core(of_core(away, 1 - core, 0, hh))
        got_here = over_core(of_core(here, 1 - core, 0, hh))
        pieces = []
        n = hh // NPIECE2
        for p in range(NPIECE2):
            sl = slice(p * n, (p + 1) * n)
            out = of_core(away, core, p * n, n) + got_away[sl]
            came = over_x(out)
            layer = (of_core(here, core, p * n, n) + got_here[sl]) + came
            pieces.append((layer + over_depth(layer)).T)
        dw_down = jnp.concatenate(pieces, axis=1)

        du = None
        for i in range(NCHUNK):
            du = du_kernel(grad, *grad_oth[i], w2, d, rows, i, du, here)

        away = dw1_kernel(jnp.stack([(1 - x + col) % 2, col, core]), x_t, du, fh, du)
        here = dw1_kernel(jnp.stack([(x + col) % 2, col, core]), x_t, du, fh, away[0])
        got_away = over_core(away[1])
        got_here = over_core(here[1])
        cols = []
        w = fh // NPIECE1
        for p in range(NPIECE1):
            sl = slice(p * w, (p + 1) * w)
            out = away[0][:, sl] + got_away[:, sl]
            came = over_x(out)
            layer = (here[0][:, sl] + got_here[:, sl]) + came
            cols.append(layer + over_depth(layer))
        dw_up = jnp.concatenate(cols, axis=1)

        dep = here[0]
        out_blk = dx_blk = None
        for p in range(NOUT):
            out_blk = out_kernel(y_body, a, w2, (w2.shape[0], hh), hh, p, NOUT, dep if p == 0 else out_blk, p > 0)
        for p in range(NOUT):
            dx_blk = out_kernel(dx_body, du, w1, (hh, w1.shape[1]), hh, p, NOUT, out_blk if p == 0 else dx_blk, p > 0)
        return out_blk, dx_blk, dw_up, dw_down

    return jax.shard_map(body, mesh=mesh, in_specs=(act_spec, weight_spec, weight_spec, act_spec),
                         out_specs=(act_spec, act_spec, weight_spec, weight_spec), check_vma=False)
```

```python
import jax
import jax.numpy as jnp
from jax import lax
from jax.experimental import pallas as pl
from jax.experimental.pallas import tpu as pltpu
from jax.sharding import PartitionSpec as P


BF16, F32 = jnp.bfloat16, jnp.float32
VMEM_LIMIT = 60 * 1024 * 1024
SQRT_2_OVER_PI = 0.7978845608028654
CUBIC = 0.044715
NCHUNK = 4
NFIRST = 2
NPIECE1 = 4
PER = 2
NSLOT = 3
PIECE = 256
TILE = 16
SUB = 512
MESH = pl.DeviceIdType.MESH
LAST_LAST = (((1,), (1,)), ((), ()))


def dot(a, b):
    return jnp.dot(a, b, preferred_element_type=F32)


def dot_t(a, b):
    return lax.dot_general(a, b, LAST_LAST, preferred_element_type=F32)


def cost(flops, nbytes, trans=0):
    return pl.CostEstimate(flops=flops, bytes_accessed=nbytes, transcendentals=trans)


def params():
    return pltpu.CompilerParams(vmem_limit_bytes=VMEM_LIMIT)


def gather_body(w1_ref, w2_ref, tok_ref, grad_ref, w1, w2, tok_oth, *rest):
    *cut, v1, v2, vt, vg, send, recv, load, store = rest
    col, row, depth = lax.axis_index("col"), lax.axis_index("row"), lax.axis_index("depth")
    x, core = row // 2, row % 2
    to_core = {"row": 2 * x + (1 - core)}
    to_x = {"row": 2 * (1 - x) + core}
    to_col = {"col": 1 - col}
    to_depth = {"depth": 1 - depth}

    barrier = pltpu.get_barrier_semaphore()
    for dev in (to_core, to_x, to_col, to_depth):
        pl.semaphore_signal(barrier, inc=1, device_id=dev, device_id_type=MESH)
    pl.semaphore_wait(barrier, 4)

    def place(which, bx, bcol, at_col, half=None):
        ref = (w1_ref, w2_ref)[which]
        n, m = ref.shape
        side = (bx + at_col) % 2 if which == 0 else (bcol + at_col) % 2
        if which == 0:
            r0, c0 = side * (2 * n) + core * n, bcol * m
        else:
            r0, c0 = (2 * bx + core) * n, side * m
        if half is not None:
            r0, n = r0 + half * (n // 2), n // 2
        return (w1, w2)[which].at[pl.ds(pl.multiple_of(r0, 32), n), pl.ds(pl.multiple_of(c0, 128), m)]

    made = []

    def start(src, dst, dev):
        i = len(made)
        cp = pltpu.make_async_remote_copy(src_ref=src, dst_ref=dst, send_sem=send.at[i], recv_sem=recv.at[i],
                                          device_id=dev, device_id_type=MESH)
        cp.start()
        made.append(cp)
        return cp

    def forward(piece, dev):
        return start(piece, piece, dev)

    def half_of(ref):
        n = ref.shape[0] // 2
        return ref.at[pl.ds(pl.multiple_of(depth * n, 32), n), :]

    late = []

    def to_partner(piece):
        late.append(forward(piece, to_core))

    other = 1 - col
    col1 = start(half_of(w1_ref), place(0, x, col, other, depth), to_col)
    x1 = start(w1_ref, place(0, x, col, col), to_x)
    col2 = start(half_of(w2_ref), place(1, x, col, other, depth), to_col)
    first = tok_oth.shape[0]
    late.append(start(tok_ref.at[pl.ds(0, first), :], tok_oth, to_col))
    late.append(start(w1_ref, place(0, x, col, col), to_core))
    late.append(start(w2_ref, place(1, x, col, col), to_core))
    size = tok_oth.shape[0] // NFIRST
    rest_of = tok_ref.shape[0] - NFIRST * size
    loads = [pltpu.make_async_copy(w1_ref, v1, load.at[0]), pltpu.make_async_copy(w2_ref, v2, load.at[1]),
             pltpu.make_async_copy(tok_ref.at[pl.ds(NFIRST * size, rest_of), :], vt, load.at[2]),
             pltpu.make_async_copy(grad_ref, vg, load.at[3])]
    for cp in loads:
        cp.start()
    for cp in loads:
        cp.wait()
    keep = [pltpu.make_async_copy(v1, place(0, x, col, col), store.at[0]),
            pltpu.make_async_copy(v2, place(1, x, col, col), store.at[1])]
    spans = [(vt, i) for i in range(NCHUNK - NFIRST)] + [(vg, i) for i in range(NCHUNK)]
    for j, (src, i) in enumerate(spans):
        keep.append(pltpu.make_async_copy(src.at[pl.ds(i * size, size), :], cut[j], store.at[2 + j]))
    for cp in keep:
        cp.start()

    def oth(which, bx, half):
        return place(which, bx, other, col, half)

    col1.wait_recv()
    z1 = forward(oth(0, x, depth), to_depth)
    x1h = forward(oth(0, x, depth), to_x)
    to_partner(oth(0, x, depth))
    x2 = start(half_of(w2_ref), place(1, x, col, col, depth), to_x)
    col2.wait_recv()
    z2 = forward(oth(1, x, depth), to_depth)
    x2h = forward(oth(1, x, depth), to_x)
    to_partner(oth(1, x, depth))
    z1.wait_recv()
    to_partner(oth(0, x, 1 - depth))
    x1.wait_recv()
    to_partner(place(0, 1 - x, col, col))
    x1h.wait_recv()
    z1d = forward(oth(0, 1 - x, depth), to_depth)
    to_partner(oth(0, 1 - x, depth))
    z2.wait_recv()
    to_partner(oth(1, x, 1 - depth))
    x2.wait_recv()
    z2o = forward(place(1, 1 - x, col, col, depth), to_depth)
    to_partner(place(1, 1 - x, col, col, depth))
    z1d.wait_recv()
    to_partner(oth(0, 1 - x, 1 - depth))
    x2h.wait_recv()
    z2d = forward(oth(1, 1 - x, depth), to_depth)
    to_partner(oth(1, 1 - x, depth))
    z2o.wait_recv()
    to_partner(place(1, 1 - x, col, col, 1 - depth))
    z2d.wait_recv()
    to_partner(oth(1, 1 - x, 1 - depth))
    for cp in late:
        cp.wait_recv()
    for cp in made:
        cp.wait_send()
    for cp in keep:
        cp.wait()


NCOPY = 25
NCUT = 2 * NCHUNK - NFIRST


def gather_kernel(up, down, tok, grad, rows):
    piece = jax.ShapeDtypeStruct((rows, tok.shape[1]), BF16)
    return pl.pallas_call(
        gather_body,
        in_specs=[pl.BlockSpec(memory_space=pl.ANY)] * 4,
        out_specs=[pl.BlockSpec(memory_space=pl.ANY)] * (3 + NCUT),
        out_shape=[jax.ShapeDtypeStruct((4 * up.shape[0], 2 * up.shape[1]), BF16),
                   jax.ShapeDtypeStruct((4 * down.shape[0], 2 * down.shape[1]), BF16),
                   jax.ShapeDtypeStruct((NFIRST * rows, tok.shape[1]), BF16)] + [piece] * NCUT,
        scratch_shapes=[pltpu.VMEM(up.shape, BF16), pltpu.VMEM(down.shape, BF16),
                        pltpu.VMEM(((NCHUNK - NFIRST) * rows, tok.shape[1]), BF16), pltpu.VMEM(grad.shape, BF16),
                        pltpu.SemaphoreType.DMA((NCOPY,)), pltpu.SemaphoreType.DMA((NCOPY,)),
                        pltpu.SemaphoreType.DMA((4,)), pltpu.SemaphoreType.DMA((2 + NCUT,))],
        compiler_params=pltpu.CompilerParams(collective_id=0, has_side_effects=True, vmem_limit_bytes=VMEM_LIMIT),
        cost_estimate=cost(0, 300_000_000),
        name="gather",
    )(up, down, tok, grad)


ANY = pl.BlockSpec(memory_space=pl.ANY)


def make_up_body(first_row, nlater):
    def up_body(xo_ref, *rest):
        xt_refs, w_ref = rest[:nlater], rest[nlater]
        a_hbm, d_hbm, x_ref, u0_ref, u1_ref, a_ref, d_ref, sem = rest[-8:]
        rows, hh = a_ref.shape[1], xo_ref.shape[1]
        piece = u0_ref.shape[0]
        last = rows // piece - 1
        bn = w_ref.shape[1]
        j, n = pl.program_id(0) * PER + pl.program_id(1), pl.num_programs(0) * PER
        row = pl.multiple_of(pl.program_id(1) * rows, rows)

        def copies(step, part):
            slot = lax.rem(step, NSLOT)
            cols = pl.ds(pl.multiple_of(lax.div(step, PER) * bn, bn), bn)
            base = pl.multiple_of(first_row + lax.rem(step, PER) * rows, rows)
            first, size = ((0, last * piece), (last * piece, piece))[part]
            src, dst = pl.ds(first, size), pl.ds(base + first, size)
            return (pltpu.make_async_copy(a_ref.at[slot, src], a_hbm.at[dst, cols], sem.at[0, part, slot]),
                    pltpu.make_async_copy(d_ref.at[slot, src], d_hbm.at[dst, cols], sem.at[1, part, slot]))

        def start(step, part):
            for cp in copies(step, part):
                cp.start()

        def wait(step, part):
            for cp in copies(step, part):
                cp.wait()

        def finish(u_ref, slot, which):
            for r in range(0, piece, TILE):
                u = u_ref[pl.ds(r, TILE), :]
                sl = pl.ds(which * piece + r, TILE)
                u2 = u * u
                t = jnp.tanh(u * (SQRT_2_OVER_PI + (SQRT_2_OVER_PI * CUBIC) * u2))
                h = 0.5 + 0.5 * t
                a_ref[slot, sl, :] = (u * h).astype(BF16)
                slope = 0.5 * SQRT_2_OVER_PI + (1.5 * SQRT_2_OVER_PI * CUBIC) * u2
                d_ref[slot, sl, :] = h + ((1.0 - t * t) * u) * slope

        @pl.when(j == 0)
        def _():
            x_ref[:, :hh] = xo_ref[...]
            at = 0
            for ref in xt_refs:
                x_ref[at:at + ref.shape[0], hh:] = ref[...]
                at += ref.shape[0]

        @pl.when(j >= NSLOT)
        def _():
            wait(j - NSLOT, 0)

        @pl.when(j >= NSLOT + 1)
        def _():
            wait(j - NSLOT - 1, 1)

        slot, prev = lax.rem(j, NSLOT), lax.rem(j + NSLOT - 1, NSLOT)
        held = (u0_ref, u1_ref)
        for i in range(last + 1):
            held[i % 2][...] = dot(x_ref[pl.ds(row + i * piece, piece), :], w_ref[...])
            if i == 0:
                finish(held[last % 2], prev, last)
            else:
                finish(held[(i - 1) % 2], slot, i - 1)
        start(j, 0)

        @pl.when(j >= 1)
        def _():
            start(j - 1, 1)

        @pl.when(j == n - 1)
        def _():
            wait(j - NSLOT, 1)
            finish(held[last % 2], slot, last)
            start(j, 1)
            for k in range(NSLOT):
                wait(j - k, 0)
                wait(j - k, 1)

    return up_body


def up_kernel(x_own, x_oth, w1, rows, call, bufs, after, bn=512):
    tokens, hh = x_own.shape
    f = w1.shape[1]
    in_specs = [pl.BlockSpec((PER * rows, hh), lambda j, i: (call, 0))]
    in_specs += [pl.BlockSpec(v.shape, lambda j, i: (0, 0)) for v in x_oth]
    in_specs += [pl.BlockSpec((2 * hh, bn), lambda j, i: (0, j))]
    args = [x_own, *x_oth, w1]
    aliases = {}
    if bufs is not None:
        aliases = {len(args): 0, len(args) + 1: 1}
        in_specs += [ANY] * 3
        args += [*bufs, after]
    return pl.pallas_call(
        make_up_body(call * PER * rows, len(x_oth)),
        grid=(f // bn, PER),
        in_specs=in_specs,
        out_specs=[ANY, ANY],
        scratch_shapes=[pltpu.VMEM((PER * rows, 2 * hh), BF16), pltpu.VMEM((PIECE, bn), F32), pltpu.VMEM((PIECE, bn), F32),
                        pltpu.VMEM((NSLOT, rows, bn), BF16), pltpu.VMEM((NSLOT, rows, bn), F32), pltpu.SemaphoreType.DMA((2, 2, NSLOT))],
        out_shape=[jax.ShapeDtypeStruct((tokens, f), BF16), jax.ShapeDtypeStruct((tokens, f), F32)],
        input_output_aliases=aliases,
        compiler_params=params(),
        cost_estimate=cost(2 * PER * rows * 2 * hh * f, PER * rows * f * 6 + 2 * hh * f * 2, PER * rows * f),
        name="up",
    )(*args)


def make_du_body(first_row, nlater):
    def du_body(go_ref, *rest):
        gt_refs, w_ref, d_hbm = rest[:nlater], rest[nlater], rest[nlater + 1]
        u_ref, g_ref, d_ref, a0_ref, a1_ref, sem = rest[-6:]
        rows, hh = u_ref.shape[0], go_ref.shape[1]
        bn = w_ref.shape[0]
        j, n = pl.program_id(0) * PER + pl.program_id(1), pl.num_programs(0) * PER
        row = pl.multiple_of(pl.program_id(1) * rows, rows)

        def copy(step):
            slot = lax.rem(step, NSLOT)
            cols = pl.ds(pl.multiple_of(lax.div(step, PER) * bn, bn), bn)
            base = pl.multiple_of(first_row + lax.rem(step, PER) * rows, rows)
            return pltpu.make_async_copy(d_hbm.at[pl.ds(base, rows), cols], d_ref.at[slot], sem.at[slot])

        @pl.when(j == 0)
        def _():
            for k in range(NSLOT - 1):
                copy(k).start()
            g_ref[:, :hh] = go_ref[...]
            at = 0
            for ref in gt_refs:
                g_ref[at:at + ref.shape[0], hh:] = ref[...]
                at += ref.shape[0]

        @pl.when(j + NSLOT - 1 < n)
        def _():
            copy(j + NSLOT - 1).start()

        copy(j).wait()
        slot = lax.rem(j, NSLOT)
        held = (a0_ref, a1_ref)
        blocks = [(i, k) for k in range(bn // SUB) for i in range(rows // SUB)]

        def finish(ref, i, k):
            for r in range(0, SUB, TILE):
                sl, sk = pl.ds(i * SUB + r, TILE), pl.ds(k * SUB, SUB)
                u_ref[sl, sk] = (ref[pl.ds(r, TILE), :] * d_ref[slot, sl, sk]).astype(BF16)

        for m, (i, k) in enumerate(blocks):
            held[m % 2][...] = dot_t(g_ref[pl.ds(row + i * SUB, SUB), :], w_ref[pl.ds(k * SUB, SUB), :])
            if m:
                finish(held[(m - 1) % 2], *blocks[m - 1])
        finish(held[(len(blocks) - 1) % 2], *blocks[-1])

    return du_body


def du_kernel(g_own, g_oth, w2, d, rows, call, buf, after, bn=1024):
    tokens, hh = g_own.shape
    f = w2.shape[0]
    in_specs = [pl.BlockSpec((PER * rows, hh), lambda j, i: (call, 0))]
    in_specs += [pl.BlockSpec(v.shape, lambda j, i: (0, 0)) for v in g_oth]
    in_specs += [pl.BlockSpec((bn, 2 * hh), lambda j, i: (j, 0)), ANY, ANY]
    args = [g_own, *g_oth, w2, d, after if buf is None else buf]
    return pl.pallas_call(
        make_du_body(call * PER * rows, len(g_oth)),
        grid=(f // bn, PER),
        in_specs=in_specs,
        out_specs=pl.BlockSpec((rows, bn), lambda j, i: (call * PER + i, j)),
        scratch_shapes=[pltpu.VMEM((PER * rows, 2 * hh), BF16), pltpu.VMEM((NSLOT, rows, bn), F32),
                        pltpu.VMEM((SUB, SUB), F32), pltpu.VMEM((SUB, SUB), F32), pltpu.SemaphoreType.DMA((NSLOT,))],
        out_shape=jax.ShapeDtypeStruct((tokens, f), BF16),
        input_output_aliases={} if buf is None else {len(args) - 1: 0},
        compiler_params=params(),
        cost_estimate=cost(2 * PER * rows * 2 * hh * f, PER * rows * f * 6 + 2 * hh * f * 2),
        name="du",
    )(*args)


def y_body(a_ref, w_ref, *rest):
    rest[-1][...] = dot(a_ref[...], w_ref[...]).astype(BF16)


def dx_body(u_ref, w_ref, *rest):
    rest[-1][...] = dot_t(w_ref[...], u_ref[...]).astype(BF16).T


def out_kernel(body, name, a, w, w_shape, hh, first, count, buf, after, bm=512):
    tokens, f = a.shape
    if name == "y":
        bm, first, count = bm // 2, 2 * first, 2 * count
    extra = [v for v in (buf, after) if v is not None]
    return pl.pallas_call(
        body,
        grid=(count,),
        in_specs=[pl.BlockSpec((bm, f), lambda i: (first + i, 0)), pl.BlockSpec(w_shape, lambda i: (0, 0))] + [ANY] * len(extra),
        out_specs=pl.BlockSpec((bm, hh), lambda i: (first + i, 0)),
        out_shape=jax.ShapeDtypeStruct((tokens, hh), BF16),
        input_output_aliases={} if buf is None else {2: 0},
        compiler_params=params(),
        cost_estimate=cost(2 * count * bm * f * hh, count * bm * f * 2 + f * hh * 2),
    )(a, w, *extra)


TR = 512


def transpose_into(t_ref, x_ref):
    for i in range(x_ref.shape[0] // TR):
        sl = pl.ds(i * TR, TR)
        t_ref[:, sl] = x_ref[sl, :].T


def dw2_body(s_ref, g_ref, a_ref, dep_ref, mine_ref, theirs_ref, t_ref, o_ref, sem):
    j, n = pl.program_id(0), pl.num_programs(0)
    m = o_ref.shape[2]

    @pl.when(j == 0)
    def _():
        transpose_into(t_ref, g_ref)

    def copy(step, u, to_ref):
        slot = lax.rem(step, 2)
        cols = lax.rem(2 * step + u, n) * m
        return pltpu.make_async_copy(o_ref.at[2 * slot + u], to_ref.at[:, pl.ds(pl.multiple_of(cols, m), m)], sem.at[slot, u])

    @pl.when(j >= 2)
    def _():
        for u in range(2):
            copy(j - 2, u, mine_ref).wait()

    slot = lax.rem(j, 2)
    r = dot(t_ref[...], a_ref[...])
    o_ref[2 * slot] = r[:, :m]
    o_ref[2 * slot + 1] = r[:, m:]
    for u in range(2):
        owner = lax.div(2 * j + u, n)

        @pl.when(owner == s_ref[1])
        def _():
            copy(j, u, mine_ref).start()

        @pl.when(owner != s_ref[1])
        def _():
            copy(j, u, theirs_ref).start()

    @pl.when(j == n - 1)
    def _():
        for k in range(2):
            for u in range(2):
                copy(j - k, u, mine_ref).wait()


def dw2_kernel(idx, g, a, width, after, bn=512):
    tokens, n = g.shape
    steps = width // bn
    shape = jax.ShapeDtypeStruct((n, width // 2), F32)
    return pl.pallas_call(
        dw2_body,
        grid_spec=pltpu.PrefetchScalarGridSpec(
            num_scalar_prefetch=1,
            grid=(steps,),
            in_specs=[
                pl.BlockSpec((tokens, n), lambda j, s: (0, 0)),
                pl.BlockSpec((tokens, bn), lambda j, s: (0, s[0] * steps + j)),
                ANY,
            ],
            out_specs=[ANY, ANY],
            scratch_shapes=[pltpu.VMEM((n, tokens), BF16), pltpu.VMEM((4, n, bn // 2), F32), pltpu.SemaphoreType.DMA((2, 2))]),
        out_shape=[shape, shape],
        compiler_params=params(),
        cost_estimate=cost(2 * tokens * n * width, tokens * (n + width) * 2 + n * width * 4),
        name="dw2",
    )(idx, g, a, after)


def dw1_body(s_ref, own_ref, *rest):
    *oth_refs, u_ref, dep_ref, mine_ref, theirs_ref, x_ref, t_ref, sem = rest

    @pl.when(pl.program_id(0) == 0)
    def _():
        @pl.when(s_ref[0] == 0)
        def _():
            cp = pltpu.make_async_copy(own_ref, x_ref, sem.at[0])
            cp.start()
            cp.wait()

        @pl.when(s_ref[0] != 0)
        def _():
            cps, at = [], 0
            for i, ref in enumerate(oth_refs):
                cps.append(pltpu.make_async_copy(ref, x_ref.at[pl.ds(at, ref.shape[0]), :], sem.at[i]))
                at += ref.shape[0]
            for cp in cps:
                cp.start()
            for cp in cps:
                cp.wait()

        transpose_into(t_ref, x_ref)

    r = dot(t_ref[...], u_ref[...])
    half = r.shape[0] // 2

    @pl.when(s_ref[2] == 0)
    def _():
        mine_ref[...] = r[:half]
        theirs_ref[...] = r[half:]

    @pl.when(s_ref[2] != 0)
    def _():
        mine_ref[...] = r[half:]
        theirs_ref[...] = r[:half]


def dw1_kernel(s, x_own, x_oth, du, width, after, bn=512):
    tokens, hh = x_own.shape
    steps = width // bn
    out_spec = pl.BlockSpec((hh // 2, bn), lambda j, s: (0, j))
    shape = jax.ShapeDtypeStruct((hh // 2, width), F32)
    return pl.pallas_call(
        dw1_body,
        grid_spec=pltpu.PrefetchScalarGridSpec(
            num_scalar_prefetch=1,
            grid=(steps,),
            in_specs=[ANY] * (1 + len(x_oth)) + [pl.BlockSpec((tokens, bn), lambda j, s: (0, s[1] * steps + j)), ANY],
            out_specs=[out_spec, out_spec],
            scratch_shapes=[pltpu.VMEM((tokens, hh), BF16), pltpu.VMEM((hh, tokens), BF16), pltpu.SemaphoreType.DMA((len(x_oth),))]),
        out_shape=[shape, shape],
        compiler_params=params(),
        cost_estimate=cost(2 * tokens * hh * width, tokens * (hh + width) * 2 + hh * width * 4),
        name="dw1",
    )(s, x_own, *x_oth, du, after)


def sum_body(here_ref, got_ref, came_ref, o_ref):
    o_ref[...] = (here_ref[...] + got_ref[...]) + came_ref[...]


def sum_kernel(here, got, came, at, steps):
    n, m = came.shape
    bm = n // steps
    plain = pl.BlockSpec((bm, m), lambda i: (i, 0))
    return pl.pallas_call(
        sum_body,
        grid=(steps,),
        in_specs=[pl.BlockSpec((bm, m), at), pl.BlockSpec((bm, m), at), plain],
        out_specs=plain,
        out_shape=jax.ShapeDtypeStruct((n, m), F32),
        compiler_params=params(),
        cost_estimate=cost(2 * n * m, 16 * n * m),
        name="layer_sum",
    )(here, got, came)


def fin2_body(*refs):
    *ins, o_ref = refs
    at = 0
    for a_ref, b_ref in zip(ins[::2], ins[1::2]):
        n = a_ref.shape[0]
        o_ref[:, at:at + n] = (a_ref[...] + b_ref[...]).T
        at += n


def fin2_kernel(pairs, bn=256):
    width = pairs[0][0].shape[1]
    flat = [v for pair in pairs for v in pair]
    n = sum(v.shape[0] for v in flat) // 2
    return pl.pallas_call(
        fin2_body,
        grid=(width // bn,),
        in_specs=[pl.BlockSpec((v.shape[0], bn), lambda j: (0, j)) for v in flat],
        out_specs=pl.BlockSpec((bn, n), lambda j: (j, 0)),
        out_shape=jax.ShapeDtypeStruct((width, n), F32),
        compiler_params=params(),
        cost_estimate=cost(n * width, 12 * n * width),
        name="fin2",
    )(*flat)


def solution(mesh):
    nx = mesh.shape["row"] // 2
    act_spec = P(("depth", "row"), "col")
    weight_spec = P("row", "col")
    pair = [(0, 1), (1, 0)]
    core_pair = [(r, r ^ 1) for r in range(2 * nx)]
    x_pair = [(r, r ^ 2) for r in range(2 * nx)]

    def over_core(v):
        return lax.ppermute(v, "row", core_pair)

    def over_x(v):
        return lax.ppermute(v, "row", x_pair)

    def over_col(v):
        return lax.ppermute(v, "col", pair)

    def over_depth(v):
        return lax.ppermute(v, "depth", pair)

    def body(tok, up, down, grad):
        col = lax.axis_index("col")
        row = lax.axis_index("row")
        x, core = row // 2, row % 2
        tokens, hh = tok.shape
        rows = tokens // NCHUNK
        fh = up.shape[1]

        w1, w2, tok_first, *cut = gather_kernel(up, down, tok, grad, rows)
        nlater = NCHUNK - NFIRST
        tok_later = [over_col(cut[i]) for i in range(nlater)]
        grad_oth = [over_col(cut[nlater + i]) for i in range(NCHUNK)]

        outs = {"y": None, "dx": None}
        parts = {"y": ((0, 4), (4, 4)), "dx": ((0, 1), (1, 1), (2, 2), (4, 4))}

        def out_part(key, part, after=None):
            args = (y_body, "y", a, w2, (w2.shape[0], hh)) if key == "y" else (dx_body, "dx", du, w1, (hh, w1.shape[1]))
            outs[key] = out_kernel(*args, hh, *parts[key][part], outs[key], after)
            return outs[key]

        a, d = up_kernel(tok, (tok_first,), w1, rows, 0, None, None)
        dep = out_part("y", 0, w1)
        a, d = up_kernel(tok, tok_later, w1, rows, 1, (a, d), dep)

        away = dw2_kernel(jnp.stack([1 - x, core]), grad, a, fh, d)
        here = dw2_kernel(jnp.stack([x, core]), grad, a, fh, away[0])
        got_away = over_core(away[1])
        got_here = over_core(here[1])
        pieces, at = [], 0
        for n in (384, hh - 384):
            came = over_x(away[0][at:at + n] + got_away[at:at + n])
            layer = sum_kernel(here[0], got_here, came, lambda i, at=at: (at // 128 + i, 0), n // 128)
            pieces.append((layer, over_depth(layer)))
            at += n
        dw_down = fin2_kernel(pieces)

        du = None
        for i in range(NCHUNK // PER):
            du = du_kernel(grad, grad_oth[i * PER:(i + 1) * PER], w2, d, rows, i, du, here[0])

        away = dw1_kernel(jnp.stack([(1 - x + col) % 2, col, core]), tok, (tok_first, *tok_later), du, fh, du)
        dep = out_part("dx", 0, away[0])
        here = dw1_kernel(jnp.stack([(x + col) % 2, col, core]), tok, (tok_first, *tok_later), du, fh, dep)
        got_away = over_core(away[1])
        got_here = over_core(here[1])
        cols = []
        w = fh // NPIECE1
        for p in range(NPIECE1):
            sl = slice(p * w, (p + 1) * w)
            out = away[0][:, sl] + got_away[:, sl]
            came = over_x(out)
            layer = sum_kernel(here[0], got_here, came, lambda i, p=p: (i, p), 2)
            cols.append(layer + over_depth(layer))
        dw_up = jnp.concatenate(cols, axis=1)

        out_part("dx", 1, here[0])
        out_part("y", 1, outs["dx"])
        out_part("dx", 2, outs["y"])
        out_part("dx", 3)
        return outs["y"], outs["dx"], dw_up, dw_down

    return jax.shard_map(body, mesh=mesh, in_specs=(act_spec, weight_spec, weight_spec, act_spec),
                         out_specs=(act_spec, act_spec, weight_spec, weight_spec), check_vma=False)
```

```python
import jax
import jax.numpy as jnp
from jax import lax
from jax.experimental import pallas as pl
from jax.experimental.pallas import tpu as pltpu
from jax.sharding import PartitionSpec as P


BF16, F32 = jnp.bfloat16, jnp.float32
VMEM_LIMIT = 60 * 1024 * 1024
SQRT_2_OVER_PI = 0.7978845608028654
CUBIC = 0.044715
NCHUNK = 4
NFIRST = 2
NPIECE1 = 4
PER = 2
NSLOT = 3
PIECE = 128
TILE = 16
SUB = 512
MESH = pl.DeviceIdType.MESH
LAST_LAST = (((1,), (1,)), ((), ()))


def dot(a, b):
    return jnp.dot(a, b, preferred_element_type=F32)


def dot_t(a, b):
    return lax.dot_general(a, b, LAST_LAST, preferred_element_type=F32)


def cost(flops, nbytes, trans=0):
    return pl.CostEstimate(flops=flops, bytes_accessed=nbytes, transcendentals=trans)


def params():
    return pltpu.CompilerParams(vmem_limit_bytes=VMEM_LIMIT)


def gather_body(w1_ref, w2_ref, tok_ref, grad_ref, w1, w2, tok_oth, *rest):
    *cut, v1, v2, vt, vg, send, recv, load, store = rest
    col, row, depth = lax.axis_index("col"), lax.axis_index("row"), lax.axis_index("depth")
    x, core = row // 2, row % 2
    to_core = {"row": 2 * x + (1 - core)}
    to_x = {"row": 2 * (1 - x) + core}
    to_col = {"col": 1 - col}
    to_depth = {"depth": 1 - depth}

    barrier = pltpu.get_barrier_semaphore()
    for dev in (to_core, to_x, to_col, to_depth):
        pl.semaphore_signal(barrier, inc=1, device_id=dev, device_id_type=MESH)
    pl.semaphore_wait(barrier, 4)

    def place(which, bx, bcol, at_col, half=None):
        ref = (w1_ref, w2_ref)[which]
        n, m = ref.shape
        side = (bx + at_col) % 2 if which == 0 else (bcol + at_col) % 2
        if which == 0:
            r0, c0 = side * (2 * n) + core * n, bcol * m
        else:
            r0, c0 = (2 * bx + core) * n, side * m
        if half is not None:
            r0, n = r0 + half * (n // 2), n // 2
        return (w1, w2)[which].at[pl.ds(pl.multiple_of(r0, 32), n), pl.ds(pl.multiple_of(c0, 128), m)]

    made = []

    def start(src, dst, dev):
        i = len(made)
        cp = pltpu.make_async_remote_copy(src_ref=src, dst_ref=dst, send_sem=send.at[i], recv_sem=recv.at[i],
                                          device_id=dev, device_id_type=MESH)
        cp.start()
        made.append(cp)
        return cp

    def forward(piece, dev):
        return start(piece, piece, dev)

    def half_of(ref):
        n = ref.shape[0] // 2
        return ref.at[pl.ds(pl.multiple_of(depth * n, 32), n), :]

    late = []

    def to_partner(piece):
        late.append(forward(piece, to_core))

    other = 1 - col
    col1 = start(half_of(w1_ref), place(0, x, col, other, depth), to_col)
    x1 = start(w1_ref, place(0, x, col, col), to_x)
    col2 = start(half_of(w2_ref), place(1, x, col, other, depth), to_col)
    first = tok_oth.shape[0]
    late.append(start(tok_ref.at[pl.ds(0, first), :], tok_oth, to_col))
    late.append(start(w1_ref, place(0, x, col, col), to_core))
    late.append(start(w2_ref, place(1, x, col, col), to_core))
    size = tok_oth.shape[0] // NFIRST
    rest_of = tok_ref.shape[0] - NFIRST * size
    loads = [pltpu.make_async_copy(w1_ref, v1, load.at[0]), pltpu.make_async_copy(w2_ref, v2, load.at[1]),
             pltpu.make_async_copy(tok_ref.at[pl.ds(NFIRST * size, rest_of), :], vt, load.at[2]),
             pltpu.make_async_copy(grad_ref, vg, load.at[3])]
    for cp in loads:
        cp.start()
    for cp in loads:
        cp.wait()
    keep = [pltpu.make_async_copy(v1, place(0, x, col, col), store.at[0]),
            pltpu.make_async_copy(v2, place(1, x, col, col), store.at[1])]
    spans = [(vt, i) for i in range(NCHUNK - NFIRST)] + [(vg, i) for i in range(NCHUNK)]
    for j, (src, i) in enumerate(spans):
        keep.append(pltpu.make_async_copy(src.at[pl.ds(i * size, size), :], cut[j], store.at[2 + j]))
    for cp in keep:
        cp.start()

    def oth(which, bx, half):
        return place(which, bx, other, col, half)

    col1.wait_recv()
    z1 = forward(oth(0, x, depth), to_depth)
    x1h = forward(oth(0, x, depth), to_x)
    to_partner(oth(0, x, depth))
    x2 = start(half_of(w2_ref), place(1, x, col, col, depth), to_x)
    col2.wait_recv()
    z2 = forward(oth(1, x, depth), to_depth)
    x2h = forward(oth(1, x, depth), to_x)
    to_partner(oth(1, x, depth))
    z1.wait_recv()
    to_partner(oth(0, x, 1 - depth))
    x1.wait_recv()
    to_partner(place(0, 1 - x, col, col))
    x1h.wait_recv()
    z1d = forward(oth(0, 1 - x, depth), to_depth)
    to_partner(oth(0, 1 - x, depth))
    z2.wait_recv()
    to_partner(oth(1, x, 1 - depth))
    x2.wait_recv()
    z2o = forward(place(1, 1 - x, col, col, depth), to_depth)
    to_partner(place(1, 1 - x, col, col, depth))
    z1d.wait_recv()
    to_partner(oth(0, 1 - x, 1 - depth))
    x2h.wait_recv()
    z2d = forward(oth(1, 1 - x, depth), to_depth)
    to_partner(oth(1, 1 - x, depth))
    z2o.wait_recv()
    to_partner(place(1, 1 - x, col, col, 1 - depth))
    z2d.wait_recv()
    to_partner(oth(1, 1 - x, 1 - depth))
    for cp in late:
        cp.wait_recv()
    for cp in made:
        cp.wait_send()
    for cp in keep:
        cp.wait()


NCOPY = 25
NCUT = 2 * NCHUNK - NFIRST


def gather_kernel(up, down, tok, grad, rows):
    piece = jax.ShapeDtypeStruct((rows, tok.shape[1]), BF16)
    return pl.pallas_call(
        gather_body,
        in_specs=[pl.BlockSpec(memory_space=pl.ANY)] * 4,
        out_specs=[pl.BlockSpec(memory_space=pl.ANY)] * (3 + NCUT),
        out_shape=[jax.ShapeDtypeStruct((4 * up.shape[0], 2 * up.shape[1]), BF16),
                   jax.ShapeDtypeStruct((4 * down.shape[0], 2 * down.shape[1]), BF16),
                   jax.ShapeDtypeStruct((NFIRST * rows, tok.shape[1]), BF16)] + [piece] * NCUT,
        scratch_shapes=[pltpu.VMEM(up.shape, BF16), pltpu.VMEM(down.shape, BF16),
                        pltpu.VMEM(((NCHUNK - NFIRST) * rows, tok.shape[1]), BF16), pltpu.VMEM(grad.shape, BF16),
                        pltpu.SemaphoreType.DMA((NCOPY,)), pltpu.SemaphoreType.DMA((NCOPY,)),
                        pltpu.SemaphoreType.DMA((4,)), pltpu.SemaphoreType.DMA((2 + NCUT,))],
        compiler_params=pltpu.CompilerParams(collective_id=0, has_side_effects=True, vmem_limit_bytes=VMEM_LIMIT),
        cost_estimate=cost(0, 300_000_000),
        name="gather",
    )(up, down, tok, grad)


ANY = pl.BlockSpec(memory_space=pl.ANY)


def make_up_body(first_row, nlater):
    def up_body(xo_ref, *rest):
        xt_refs, w_ref = rest[:nlater], rest[nlater]
        a_hbm, d_hbm, x_ref, u0_ref, u1_ref, a_ref, d_ref, sem = rest[-8:]
        rows, hh = a_ref.shape[1], xo_ref.shape[1]
        piece = u0_ref.shape[0]
        last = rows // piece - 1
        bn = w_ref.shape[1]
        j, n = pl.program_id(0) * PER + pl.program_id(1), pl.num_programs(0) * PER
        row = pl.multiple_of(pl.program_id(1) * rows, rows)

        def copies(step, part):
            slot = lax.rem(step, NSLOT)
            cols = pl.ds(pl.multiple_of(lax.div(step, PER) * bn, bn), bn)
            base = pl.multiple_of(first_row + lax.rem(step, PER) * rows, rows)
            first, size = ((0, last * piece), (last * piece, piece))[part]
            src, dst = pl.ds(first, size), pl.ds(base + first, size)
            return (pltpu.make_async_copy(a_ref.at[slot, src], a_hbm.at[dst, cols], sem.at[0, part, slot]),
                    pltpu.make_async_copy(d_ref.at[slot, src], d_hbm.at[dst, cols], sem.at[1, part, slot]))

        def start(step, part):
            for cp in copies(step, part):
                cp.start()

        def wait(step, part):
            for cp in copies(step, part):
                cp.wait()

        def finish(u_ref, slot, which):
            for r in range(0, piece, TILE):
                u = u_ref[pl.ds(r, TILE), :]
                sl = pl.ds(which * piece + r, TILE)
                u2 = u * u
                t = jnp.tanh(u * (SQRT_2_OVER_PI + (SQRT_2_OVER_PI * CUBIC) * u2))
                h = 0.5 + 0.5 * t
                act = u * h
                a_ref[slot, sl, :] = act.astype(BF16)
                slope = 2.0 * SQRT_2_OVER_PI + (6.0 * SQRT_2_OVER_PI * CUBIC) * u2
                d_ref[slot, sl, :] = h + (h * (u - act)) * slope

        @pl.when(j == 0)
        def _():
            x_ref[:, :hh] = xo_ref[...]
            at = 0
            for ref in xt_refs:
                x_ref[at:at + ref.shape[0], hh:] = ref[...]
                at += ref.shape[0]

        @pl.when(j >= NSLOT)
        def _():
            wait(j - NSLOT, 0)

        @pl.when(j >= NSLOT + 1)
        def _():
            wait(j - NSLOT - 1, 1)

        slot, prev = lax.rem(j, NSLOT), lax.rem(j + NSLOT - 1, NSLOT)
        held = (u0_ref, u1_ref)
        for i in range(last + 1):
            held[i % 2][...] = dot(x_ref[pl.ds(row + i * piece, piece), :], w_ref[...])
            if i == 0:
                finish(held[last % 2], prev, last)
            else:
                finish(held[(i - 1) % 2], slot, i - 1)
        start(j, 0)

        @pl.when(j >= 1)
        def _():
            start(j - 1, 1)

        @pl.when(j == n - 1)
        def _():
            wait(j - NSLOT, 1)
            finish(held[last % 2], slot, last)
            start(j, 1)
            for k in range(NSLOT):
                wait(j - k, 0)
                wait(j - k, 1)

    return up_body


def up_kernel(x_own, x_oth, w1, rows, call, bufs, after, bn=512):
    tokens, hh = x_own.shape
    f = w1.shape[1]
    in_specs = [pl.BlockSpec((PER * rows, hh), lambda j, i: (call, 0))]
    in_specs += [pl.BlockSpec(v.shape, lambda j, i: (0, 0)) for v in x_oth]
    in_specs += [pl.BlockSpec((2 * hh, bn), lambda j, i: (0, j))]
    args = [x_own, *x_oth, w1]
    aliases = {}
    if bufs is not None:
        aliases = {len(args): 0, len(args) + 1: 1}
        in_specs += [ANY] * 3
        args += [*bufs, after]
    return pl.pallas_call(
        make_up_body(call * PER * rows, len(x_oth)),
        grid=(f // bn, PER),
        in_specs=in_specs,
        out_specs=[ANY, ANY],
        scratch_shapes=[pltpu.VMEM((PER * rows, 2 * hh), BF16), pltpu.VMEM((PIECE, bn), F32), pltpu.VMEM((PIECE, bn), F32),
                        pltpu.VMEM((NSLOT, rows, bn), BF16), pltpu.VMEM((NSLOT, rows, bn), F32), pltpu.SemaphoreType.DMA((2, 2, NSLOT))],
        out_shape=[jax.ShapeDtypeStruct((tokens, f), BF16), jax.ShapeDtypeStruct((tokens, f), F32)],
        input_output_aliases=aliases,
        compiler_params=params(),
        cost_estimate=cost(2 * PER * rows * 2 * hh * f, PER * rows * f * 6 + 2 * hh * f * 2, PER * rows * f),
        name="up",
    )(*args)


def make_du_body(first_row, nlater):
    def du_body(go_ref, *rest):
        gt_refs, w_ref, d_hbm = rest[:nlater], rest[nlater], rest[nlater + 1]
        u_ref, g_ref, d_ref, a0_ref, a1_ref, sem = rest[-6:]
        rows, hh = u_ref.shape[0], go_ref.shape[1]
        bn = w_ref.shape[0]
        j, n = pl.program_id(0) * PER + pl.program_id(1), pl.num_programs(0) * PER
        row = pl.multiple_of(pl.program_id(1) * rows, rows)

        def copy(step):
            slot = lax.rem(step, NSLOT)
            cols = pl.ds(pl.multiple_of(lax.div(step, PER) * bn, bn), bn)
            base = pl.multiple_of(first_row + lax.rem(step, PER) * rows, rows)
            return pltpu.make_async_copy(d_hbm.at[pl.ds(base, rows), cols], d_ref.at[slot], sem.at[slot])

        @pl.when(j == 0)
        def _():
            for k in range(NSLOT - 1):
                copy(k).start()
            g_ref[:, :hh] = go_ref[...]
            at = 0
            for ref in gt_refs:
                g_ref[at:at + ref.shape[0], hh:] = ref[...]
                at += ref.shape[0]

        @pl.when(j + NSLOT - 1 < n)
        def _():
            copy(j + NSLOT - 1).start()

        copy(j).wait()
        slot = lax.rem(j, NSLOT)
        held = (a0_ref, a1_ref)
        blocks = [(i, k) for k in range(bn // SUB) for i in range(rows // SUB)]

        def finish(ref, i, k):
            for r in range(0, SUB, TILE):
                sl, sk = pl.ds(i * SUB + r, TILE), pl.ds(k * SUB, SUB)
                u_ref[sl, sk] = (ref[pl.ds(r, TILE), :] * d_ref[slot, sl, sk]).astype(BF16)

        for m, (i, k) in enumerate(blocks):
            held[m % 2][...] = dot_t(g_ref[pl.ds(row + i * SUB, SUB), :], w_ref[pl.ds(k * SUB, SUB), :])
            if m:
                finish(held[(m - 1) % 2], *blocks[m - 1])
        finish(held[(len(blocks) - 1) % 2], *blocks[-1])

    return du_body


def du_kernel(g_own, g_oth, w2, d, rows, call, buf, after, bn=1024):
    tokens, hh = g_own.shape
    f = w2.shape[0]
    in_specs = [pl.BlockSpec((PER * rows, hh), lambda j, i: (call, 0))]
    in_specs += [pl.BlockSpec(v.shape, lambda j, i: (0, 0)) for v in g_oth]
    in_specs += [pl.BlockSpec((bn, 2 * hh), lambda j, i: (j, 0)), ANY, ANY]
    args = [g_own, *g_oth, w2, d, after if buf is None else buf]
    return pl.pallas_call(
        make_du_body(call * PER * rows, len(g_oth)),
        grid=(f // bn, PER),
        in_specs=in_specs,
        out_specs=pl.BlockSpec((rows, bn), lambda j, i: (call * PER + i, j)),
        scratch_shapes=[pltpu.VMEM((PER * rows, 2 * hh), BF16), pltpu.VMEM((NSLOT, rows, bn), F32),
                        pltpu.VMEM((SUB, SUB), F32), pltpu.VMEM((SUB, SUB), F32), pltpu.SemaphoreType.DMA((NSLOT,))],
        out_shape=jax.ShapeDtypeStruct((tokens, f), BF16),
        input_output_aliases={} if buf is None else {len(args) - 1: 0},
        compiler_params=params(),
        cost_estimate=cost(2 * PER * rows * 2 * hh * f, PER * rows * f * 6 + 2 * hh * f * 2),
        name="du",
    )(*args)


def y_body(a_ref, w_ref, *rest):
    rest[-1][...] = dot(a_ref[...], w_ref[...]).astype(BF16)


def dx_body(u_ref, w_ref, *rest):
    rest[-1][...] = dot_t(w_ref[...], u_ref[...]).astype(BF16).T


def out_kernel(body, name, a, w, w_shape, hh, first, count, buf, after, bm=512):
    tokens, f = a.shape
    if name == "y":
        bm, first, count = bm // 2, 2 * first, 2 * count
    extra = [v for v in (buf, after) if v is not None]
    return pl.pallas_call(
        body,
        grid=(count,),
        in_specs=[pl.BlockSpec((bm, f), lambda i: (first + i, 0)), pl.BlockSpec(w_shape, lambda i: (0, 0))] + [ANY] * len(extra),
        out_specs=pl.BlockSpec((bm, hh), lambda i: (first + i, 0)),
        out_shape=jax.ShapeDtypeStruct((tokens, hh), BF16),
        input_output_aliases={} if buf is None else {2: 0},
        compiler_params=params(),
        cost_estimate=cost(2 * count * bm * f * hh, count * bm * f * 2 + f * hh * 2),
    )(a, w, *extra)


TR = 512


def transpose_into(t_ref, x_ref):
    for i in range(x_ref.shape[0] // TR):
        sl = pl.ds(i * TR, TR)
        t_ref[:, sl] = x_ref[sl, :].T


def dw2_body(s_ref, g_ref, a_ref, dep_ref, mine_ref, theirs_ref, t_ref, o_ref, sem):
    j, n = pl.program_id(0), pl.num_programs(0)
    m = o_ref.shape[2]

    @pl.when(j == 0)
    def _():
        transpose_into(t_ref, g_ref)

    def copy(step, u, to_ref):
        slot = lax.rem(step, 2)
        cols = lax.rem(2 * step + u, n) * m
        return pltpu.make_async_copy(o_ref.at[2 * slot + u], to_ref.at[:, pl.ds(pl.multiple_of(cols, m), m)], sem.at[slot, u])

    @pl.when(j >= 2)
    def _():
        for u in range(2):
            copy(j - 2, u, mine_ref).wait()

    slot = lax.rem(j, 2)
    r = dot(t_ref[...], a_ref[...])
    o_ref[2 * slot] = r[:, :m]
    o_ref[2 * slot + 1] = r[:, m:]
    for u in range(2):
        owner = lax.div(2 * j + u, n)

        @pl.when(owner == s_ref[1])
        def _():
            copy(j, u, mine_ref).start()

        @pl.when(owner != s_ref[1])
        def _():
            copy(j, u, theirs_ref).start()

    @pl.when(j == n - 1)
    def _():
        for k in range(2):
            for u in range(2):
                copy(j - k, u, mine_ref).wait()


def dw2_kernel(idx, g, a, width, after, bn=512):
    tokens, n = g.shape
    steps = width // bn
    shape = jax.ShapeDtypeStruct((n, width // 2), F32)
    return pl.pallas_call(
        dw2_body,
        grid_spec=pltpu.PrefetchScalarGridSpec(
            num_scalar_prefetch=1,
            grid=(steps,),
            in_specs=[
                pl.BlockSpec((tokens, n), lambda j, s: (0, 0)),
                pl.BlockSpec((tokens, bn), lambda j, s: (0, s[0] * steps + j)),
                ANY,
            ],
            out_specs=[ANY, ANY],
            scratch_shapes=[pltpu.VMEM((n, tokens), BF16), pltpu.VMEM((4, n, bn // 2), F32), pltpu.SemaphoreType.DMA((2, 2))]),
        out_shape=[shape, shape],
        compiler_params=params(),
        cost_estimate=cost(2 * tokens * n * width, tokens * (n + width) * 2 + n * width * 4),
        name="dw2",
    )(idx, g, a, after)


def dw1_body(s_ref, own_ref, *rest):
    *oth_refs, u_ref, dep_ref, mine_ref, theirs_ref, x_ref, t_ref, sem = rest

    @pl.when(pl.program_id(0) == 0)
    def _():
        @pl.when(s_ref[0] == 0)
        def _():
            cp = pltpu.make_async_copy(own_ref, x_ref, sem.at[0])
            cp.start()
            cp.wait()

        @pl.when(s_ref[0] != 0)
        def _():
            cps, at = [], 0
            for i, ref in enumerate(oth_refs):
                cps.append(pltpu.make_async_copy(ref, x_ref.at[pl.ds(at, ref.shape[0]), :], sem.at[i]))
                at += ref.shape[0]
            for cp in cps:
                cp.start()
            for cp in cps:
                cp.wait()

        transpose_into(t_ref, x_ref)

    r = dot(t_ref[...], u_ref[...])
    half = r.shape[0] // 2

    @pl.when(s_ref[2] == 0)
    def _():
        mine_ref[...] = r[:half]
        theirs_ref[...] = r[half:]

    @pl.when(s_ref[2] != 0)
    def _():
        mine_ref[...] = r[half:]
        theirs_ref[...] = r[:half]


def dw1_kernel(s, x_own, x_oth, du, width, after, bn=512):
    tokens, hh = x_own.shape
    steps = width // bn
    out_spec = pl.BlockSpec((hh // 2, bn), lambda j, s: (0, j))
    shape = jax.ShapeDtypeStruct((hh // 2, width), F32)
    return pl.pallas_call(
        dw1_body,
        grid_spec=pltpu.PrefetchScalarGridSpec(
            num_scalar_prefetch=1,
            grid=(steps,),
            in_specs=[ANY] * (1 + len(x_oth)) + [pl.BlockSpec((tokens, bn), lambda j, s: (0, s[1] * steps + j)), ANY],
            out_specs=[out_spec, out_spec],
            scratch_shapes=[pltpu.VMEM((tokens, hh), BF16), pltpu.VMEM((hh, tokens), BF16), pltpu.SemaphoreType.DMA((len(x_oth),))]),
        out_shape=[shape, shape],
        compiler_params=params(),
        cost_estimate=cost(2 * tokens * hh * width, tokens * (hh + width) * 2 + hh * width * 4),
        name="dw1",
    )(s, x_own, *x_oth, du, after)


def sum_body(here_ref, got_ref, came_ref, o_ref):
    o_ref[...] = (here_ref[...] + got_ref[...]) + came_ref[...]


def sum_kernel(here, got, came, at, steps):
    n, m = came.shape
    bm = n // steps
    plain = pl.BlockSpec((bm, m), lambda i: (i, 0))
    return pl.pallas_call(
        sum_body,
        grid=(steps,),
        in_specs=[pl.BlockSpec((bm, m), at), pl.BlockSpec((bm, m), at), plain],
        out_specs=plain,
        out_shape=jax.ShapeDtypeStruct((n, m), F32),
        compiler_params=params(),
        cost_estimate=cost(2 * n * m, 16 * n * m),
        name="layer_sum",
    )(here, got, came)


def fin2_body(*refs):
    *ins, o_ref = refs
    at = 0
    for a_ref, b_ref in zip(ins[::2], ins[1::2]):
        n = a_ref.shape[0]
        o_ref[:, at:at + n] = (a_ref[...] + b_ref[...]).T
        at += n


def fin2_kernel(pairs, bn=256):
    width = pairs[0][0].shape[1]
    flat = [v for pair in pairs for v in pair]
    n = sum(v.shape[0] for v in flat) // 2
    return pl.pallas_call(
        fin2_body,
        grid=(width // bn,),
        in_specs=[pl.BlockSpec((v.shape[0], bn), lambda j: (0, j)) for v in flat],
        out_specs=pl.BlockSpec((bn, n), lambda j: (j, 0)),
        out_shape=jax.ShapeDtypeStruct((width, n), F32),
        compiler_params=params(),
        cost_estimate=cost(n * width, 12 * n * width),
        name="fin2",
    )(*flat)


def solution(mesh):
    nx = mesh.shape["row"] // 2
    act_spec = P(("depth", "row"), "col")
    weight_spec = P("row", "col")
    pair = [(0, 1), (1, 0)]
    core_pair = [(r, r ^ 1) for r in range(2 * nx)]
    x_pair = [(r, r ^ 2) for r in range(2 * nx)]

    def over_core(v):
        return lax.ppermute(v, "row", core_pair)

    def over_x(v):
        return lax.ppermute(v, "row", x_pair)

    def over_col(v):
        return lax.ppermute(v, "col", pair)

    def over_depth(v):
        return lax.ppermute(v, "depth", pair)

    def body(tok, up, down, grad):
        col = lax.axis_index("col")
        row = lax.axis_index("row")
        x, core = row // 2, row % 2
        tokens, hh = tok.shape
        rows = tokens // NCHUNK
        fh = up.shape[1]

        w1, w2, tok_first, *cut = gather_kernel(up, down, tok, grad, rows)
        nlater = NCHUNK - NFIRST
        tok_later = [over_col(cut[i]) for i in range(nlater)]
        grad_oth = [over_col(cut[nlater + i]) for i in range(NCHUNK)]

        outs = {"y": None, "dx": None}
        parts = {"y": ((0, 4), (4, 2), (6, 2)), "dx": ((0, 1), (1, 3), (4, 4))}

        def out_part(key, part, after=None):
            args = (y_body, "y", a, w2, (w2.shape[0], hh)) if key == "y" else (dx_body, "dx", du, w1, (hh, w1.shape[1]))
            outs[key] = out_kernel(*args, hh, *parts[key][part], outs[key], after)
            return outs[key]

        a, d = up_kernel(tok, (tok_first,), w1, rows, 0, None, None)
        dep = out_part("y", 0, w1)
        a, d = up_kernel(tok, tok_later, w1, rows, 1, (a, d), dep)

        away = dw2_kernel(jnp.stack([1 - x, core]), grad, a, fh, d)
        here = dw2_kernel(jnp.stack([x, core]), grad, a, fh, away[0])
        got_away = over_core(away[1])
        got_here = over_core(here[1])
        pieces, at = [], 0
        for n in (256, hh - 256):
            came = over_x(away[0][at:at + n] + got_away[at:at + n])
            layer = sum_kernel(here[0], got_here, came, lambda i, at=at: (at // 128 + i, 0), n // 128)
            pieces.append((layer, over_depth(layer)))
            at += n
        dw_down = fin2_kernel(pieces)

        du = None
        for i in range(NCHUNK // PER):
            du = du_kernel(grad, grad_oth[i * PER:(i + 1) * PER], w2, d, rows, i, du, here[0])

        away = dw1_kernel(jnp.stack([(1 - x + col) % 2, col, core]), tok, (tok_first, *tok_later), du, fh, du)
        here = dw1_kernel(jnp.stack([(x + col) % 2, col, core]), tok, (tok_first, *tok_later), du, fh, away[0])
        got_away = over_core(away[1])
        got_here = over_core(here[1])
        cols = []
        w = fh // NPIECE1
        for p in range(NPIECE1):
            sl = slice(p * w, (p + 1) * w)
            out = away[0][:, sl] + got_away[:, sl]
            came = over_x(out)
            layer = sum_kernel(here[0], got_here, came, lambda i, p=p: (i, p), 2)
            cols.append(layer + over_depth(layer))
        dw_up = jnp.concatenate(cols, axis=1)

        out_part("dx", 0, here[0])
        out_part("y", 1, outs["dx"])
        out_part("y", 2)
        out_part("dx", 1, outs["y"])
        out_part("dx", 2)
        return outs["y"], outs["dx"], dw_up, dw_down

    return jax.shard_map(body, mesh=mesh, in_specs=(act_spec, weight_spec, weight_spec, act_spec),
                         out_specs=(act_spec, act_spec, weight_spec, weight_spec), check_vma=False)
```

```python
import jax
import jax.numpy as jnp
from jax import lax
from jax.experimental import pallas as pl
from jax.experimental.pallas import tpu as pltpu
from jax.sharding import PartitionSpec as P


BF16, F32 = jnp.bfloat16, jnp.float32
VMEM_LIMIT = 60 * 1024 * 1024
SQRT_2_OVER_PI = 0.7978845608028654
CUBIC = 0.044715
NHALF = 2
NPIECE1 = 4
PER = 2
NSLOT = 3
PIECE = 128
TILE = 16
SUB = 512
MESH = pl.DeviceIdType.MESH
LAST_LAST = (((1,), (1,)), ((), ()))


def dot(a, b):
    return jnp.dot(a, b, preferred_element_type=F32)


def dot_t(a, b):
    return lax.dot_general(a, b, LAST_LAST, preferred_element_type=F32)


def cost(flops, nbytes, trans=0):
    return pl.CostEstimate(flops=flops, bytes_accessed=nbytes, transcendentals=trans)


def params():
    return pltpu.CompilerParams(vmem_limit_bytes=VMEM_LIMIT)


def gather_body(w1_ref, w2_ref, tok_ref, grad_ref, w1, w2, tok_oth, *rest):
    *cut, v1, v2, vt, vg, send, recv, load, store = rest
    col, row, depth = lax.axis_index("col"), lax.axis_index("row"), lax.axis_index("depth")
    x, core = row // 2, row % 2
    to_core = {"row": 2 * x + (1 - core)}
    to_x = {"row": 2 * (1 - x) + core}
    to_col = {"col": 1 - col}
    to_depth = {"depth": 1 - depth}

    barrier = pltpu.get_barrier_semaphore()
    for dev in (to_core, to_x, to_col, to_depth):
        pl.semaphore_signal(barrier, inc=1, device_id=dev, device_id_type=MESH)
    pl.semaphore_wait(barrier, 4)

    def place(which, bx, bcol, at_col, half=None):
        ref = (w1_ref, w2_ref)[which]
        n, m = ref.shape
        side = (bx + at_col) % 2 if which == 0 else (bcol + at_col) % 2
        if which == 0:
            r0, c0 = side * (2 * n) + core * n, bcol * m
        else:
            r0, c0 = (2 * bx + core) * n, side * m
        if half is not None:
            r0, n = r0 + half * (n // 2), n // 2
        return (w1, w2)[which].at[pl.ds(pl.multiple_of(r0, 32), n), pl.ds(pl.multiple_of(c0, 128), m)]

    made = []

    def start(src, dst, dev):
        i = len(made)
        cp = pltpu.make_async_remote_copy(src_ref=src, dst_ref=dst, send_sem=send.at[i], recv_sem=recv.at[i],
                                          device_id=dev, device_id_type=MESH)
        cp.start()
        made.append(cp)
        return cp

    def forward(piece, dev):
        return start(piece, piece, dev)

    def half_of(ref):
        n = ref.shape[0] // 2
        return ref.at[pl.ds(pl.multiple_of(depth * n, 32), n), :]

    late = []

    def to_partner(piece):
        late.append(forward(piece, to_core))

    other = 1 - col
    col1 = start(half_of(w1_ref), place(0, x, col, other, depth), to_col)
    x1 = start(w1_ref, place(0, x, col, col), to_x)
    col2 = start(half_of(w2_ref), place(1, x, col, other, depth), to_col)
    first = tok_oth.shape[0]
    late.append(start(tok_ref.at[pl.ds(0, first), :], tok_oth, to_col))
    late.append(start(w1_ref, place(0, x, col, col), to_core))
    late.append(start(w2_ref, place(1, x, col, col), to_core))
    size = tok_oth.shape[0]
    loads = [pltpu.make_async_copy(w1_ref, v1, load.at[0]), pltpu.make_async_copy(w2_ref, v2, load.at[1]),
             pltpu.make_async_copy(tok_ref.at[pl.ds(size, size), :], vt, load.at[2]),
             pltpu.make_async_copy(grad_ref, vg, load.at[3])]
    for cp in loads:
        cp.start()
    for cp in loads:
        cp.wait()
    keep = [pltpu.make_async_copy(v1, place(0, x, col, col), store.at[0]),
            pltpu.make_async_copy(v2, place(1, x, col, col), store.at[1])]
    spans = [(vt, 0)] + [(vg, i) for i in range(NHALF)]
    for j, (src, i) in enumerate(spans):
        keep.append(pltpu.make_async_copy(src.at[pl.ds(i * size, size), :], cut[j], store.at[2 + j]))
    for cp in keep:
        cp.start()

    def oth(which, bx, half):
        return place(which, bx, other, col, half)

    col1.wait_recv()
    z1 = forward(oth(0, x, depth), to_depth)
    x1h = forward(oth(0, x, depth), to_x)
    to_partner(oth(0, x, depth))
    x2 = start(half_of(w2_ref), place(1, x, col, col, depth), to_x)
    col2.wait_recv()
    z2 = forward(oth(1, x, depth), to_depth)
    x2h = forward(oth(1, x, depth), to_x)
    to_partner(oth(1, x, depth))
    z1.wait_recv()
    to_partner(oth(0, x, 1 - depth))
    x1.wait_recv()
    to_partner(place(0, 1 - x, col, col))
    x1h.wait_recv()
    z1d = forward(oth(0, 1 - x, depth), to_depth)
    to_partner(oth(0, 1 - x, depth))
    z2.wait_recv()
    to_partner(oth(1, x, 1 - depth))
    x2.wait_recv()
    z2o = forward(place(1, 1 - x, col, col, depth), to_depth)
    to_partner(place(1, 1 - x, col, col, depth))
    z1d.wait_recv()
    to_partner(oth(0, 1 - x, 1 - depth))
    x2h.wait_recv()
    z2d = forward(oth(1, 1 - x, depth), to_depth)
    to_partner(oth(1, 1 - x, depth))
    z2o.wait_recv()
    to_partner(place(1, 1 - x, col, col, 1 - depth))
    z2d.wait_recv()
    to_partner(oth(1, 1 - x, 1 - depth))
    for cp in late:
        cp.wait_recv()
    for cp in made:
        cp.wait_send()
    for cp in keep:
        cp.wait()


NCOPY = 25
NCUT = 1 + NHALF


def gather_kernel(up, down, tok, grad, rows):
    piece = jax.ShapeDtypeStruct((rows, tok.shape[1]), BF16)
    return pl.pallas_call(
        gather_body,
        in_specs=[pl.BlockSpec(memory_space=pl.ANY)] * 4,
        out_specs=[pl.BlockSpec(memory_space=pl.ANY)] * (3 + NCUT),
        out_shape=[jax.ShapeDtypeStruct((4 * up.shape[0], 2 * up.shape[1]), BF16),
                   jax.ShapeDtypeStruct((4 * down.shape[0], 2 * down.shape[1]), BF16),
                   piece] + [piece] * NCUT,
        scratch_shapes=[pltpu.VMEM(up.shape, BF16), pltpu.VMEM(down.shape, BF16),
                        pltpu.VMEM((rows, tok.shape[1]), BF16), pltpu.VMEM(grad.shape, BF16),
                        pltpu.SemaphoreType.DMA((NCOPY,)), pltpu.SemaphoreType.DMA((NCOPY,)),
                        pltpu.SemaphoreType.DMA((4,)), pltpu.SemaphoreType.DMA((2 + NCUT,))],
        compiler_params=pltpu.CompilerParams(collective_id=0, has_side_effects=True, vmem_limit_bytes=VMEM_LIMIT),
        cost_estimate=cost(0, 300_000_000),
        name="gather",
    )(up, down, tok, grad)


ANY = pl.BlockSpec(memory_space=pl.ANY)


def make_up_body(first_row, nlater, per):
    def up_body(xo_ref, *rest):
        xt_refs, w_ref = rest[:nlater], rest[nlater]
        a_hbm, d_hbm, x_ref, u0_ref, u1_ref, a_ref, d_ref, sem = rest[-8:]
        rows, hh = a_ref.shape[1], xo_ref.shape[1]
        piece = u0_ref.shape[0]
        last = rows // piece - 1
        bn = w_ref.shape[1]
        j, n = pl.program_id(0) * per + pl.program_id(1), pl.num_programs(0) * per
        row = pl.multiple_of(pl.program_id(1) * rows, rows)

        def copies(step, part):
            slot = lax.rem(step, NSLOT)
            cols = pl.ds(pl.multiple_of(lax.div(step, per) * bn, bn), bn)
            base = pl.multiple_of(first_row + lax.rem(step, per) * rows, rows)
            first, size = ((0, last * piece), (last * piece, piece))[part]
            src, dst = pl.ds(first, size), pl.ds(base + first, size)
            return (pltpu.make_async_copy(a_ref.at[slot, src], a_hbm.at[dst, cols], sem.at[0, part, slot]),
                    pltpu.make_async_copy(d_ref.at[slot, src], d_hbm.at[dst, cols], sem.at[1, part, slot]))

        def start(step, part):
            for cp in copies(step, part):
                cp.start()

        def wait(step, part):
            for cp in copies(step, part):
                cp.wait()

        def finish(u_ref, slot, which):
            for r in range(0, piece, TILE):
                u = u_ref[pl.ds(r, TILE), :]
                sl = pl.ds(which * piece + r, TILE)
                u2 = u * u
                t = jnp.tanh(u * (SQRT_2_OVER_PI + (SQRT_2_OVER_PI * CUBIC) * u2))
                h = 0.5 + 0.5 * t
                act = u * h
                a_ref[slot, sl, :] = act.astype(BF16)
                slope = 2.0 * SQRT_2_OVER_PI + (6.0 * SQRT_2_OVER_PI * CUBIC) * u2
                d_ref[slot, sl, :] = h + (h * (u - act)) * slope

        @pl.when(j == 0)
        def _():
            x_ref[:, :hh] = xo_ref[...]
            at = 0
            for ref in xt_refs:
                x_ref[at:at + ref.shape[0], hh:] = ref[...]
                at += ref.shape[0]

        @pl.when(j >= NSLOT)
        def _():
            wait(j - NSLOT, 0)

        @pl.when(j >= NSLOT + 1)
        def _():
            wait(j - NSLOT - 1, 1)

        slot, prev = lax.rem(j, NSLOT), lax.rem(j + NSLOT - 1, NSLOT)
        held = (u0_ref, u1_ref)
        for i in range(last + 1):
            held[i % 2][...] = dot(x_ref[pl.ds(row + i * piece, piece), :], w_ref[...])
            if i == 0:
                finish(held[last % 2], prev, last)
            else:
                finish(held[(i - 1) % 2], slot, i - 1)
        start(j, 0)

        @pl.when(j >= 1)
        def _():
            start(j - 1, 1)

        @pl.when(j == n - 1)
        def _():
            wait(j - NSLOT, 1)
            finish(held[last % 2], slot, last)
            start(j, 1)
            for k in range(NSLOT):
                wait(j - k, 0)
                wait(j - k, 1)

    return up_body


def up_kernel(x_own, x_oth, w1, call, bufs, after, rows=512, bn=1024):
    tokens, hh = x_own.shape
    f = w1.shape[1]
    total = sum(v.shape[0] for v in x_oth)
    in_specs = [pl.BlockSpec((total, hh), lambda j, i: (call, 0))]
    in_specs += [pl.BlockSpec(v.shape, lambda j, i: (0, 0)) for v in x_oth]
    in_specs += [pl.BlockSpec((2 * hh, bn), lambda j, i: (0, j))]
    args = [x_own, *x_oth, w1]
    aliases = {}
    if bufs is not None:
        aliases = {len(args): 0, len(args) + 1: 1}
        in_specs += [ANY] * 3
        args += [*bufs, after]
    return pl.pallas_call(
        make_up_body(call * total, len(x_oth), total // rows),
        grid=(f // bn, total // rows),
        in_specs=in_specs,
        out_specs=[ANY, ANY],
        scratch_shapes=[pltpu.VMEM((total, 2 * hh), BF16), pltpu.VMEM((PIECE, bn), F32), pltpu.VMEM((PIECE, bn), F32),
                        pltpu.VMEM((NSLOT, rows, bn), BF16), pltpu.VMEM((NSLOT, rows, bn), F32), pltpu.SemaphoreType.DMA((2, 2, NSLOT))],
        out_shape=[jax.ShapeDtypeStruct((tokens, f), BF16), jax.ShapeDtypeStruct((tokens, f), F32)],
        input_output_aliases=aliases,
        compiler_params=params(),
        cost_estimate=cost(2 * total * 2 * hh * f, total * f * 6 + 2 * hh * f * 2, total * f),
        name="up",
    )(*args)


def make_du_body(first_row, nlater):
    def du_body(go_ref, *rest):
        gt_refs, w_ref, d_hbm = rest[:nlater], rest[nlater], rest[nlater + 1]
        u_ref, g_ref, d_ref, a0_ref, a1_ref, sem = rest[-6:]
        rows, hh = u_ref.shape[0], go_ref.shape[1]
        bn = w_ref.shape[0]
        j, n = pl.program_id(0) * PER + pl.program_id(1), pl.num_programs(0) * PER
        row = pl.multiple_of(pl.program_id(1) * rows, rows)

        def copy(step):
            slot = lax.rem(step, NSLOT)
            cols = pl.ds(pl.multiple_of(lax.div(step, PER) * bn, bn), bn)
            base = pl.multiple_of(first_row + lax.rem(step, PER) * rows, rows)
            return pltpu.make_async_copy(d_hbm.at[pl.ds(base, rows), cols], d_ref.at[slot], sem.at[slot])

        @pl.when(j == 0)
        def _():
            for k in range(NSLOT - 1):
                copy(k).start()
            g_ref[:, :hh] = go_ref[...]
            at = 0
            for ref in gt_refs:
                g_ref[at:at + ref.shape[0], hh:] = ref[...]
                at += ref.shape[0]

        @pl.when(j + NSLOT - 1 < n)
        def _():
            copy(j + NSLOT - 1).start()

        copy(j).wait()
        slot = lax.rem(j, NSLOT)
        held = (a0_ref, a1_ref)
        blocks = [(i, k) for k in range(bn // SUB) for i in range(rows // SUB)]

        def finish(ref, i, k):
            for r in range(0, SUB, TILE):
                sl, sk = pl.ds(i * SUB + r, TILE), pl.ds(k * SUB, SUB)
                u_ref[sl, sk] = (ref[pl.ds(r, TILE), :] * d_ref[slot, sl, sk]).astype(BF16)

        for m, (i, k) in enumerate(blocks):
            held[m % 2][...] = dot_t(g_ref[pl.ds(row + i * SUB, SUB), :], w_ref[pl.ds(k * SUB, SUB), :])
            if m:
                finish(held[(m - 1) % 2], *blocks[m - 1])
        finish(held[(len(blocks) - 1) % 2], *blocks[-1])

    return du_body


def du_kernel(g_own, g_oth, w2, d, rows, call, buf, after, bn=1024):
    tokens, hh = g_own.shape
    f = w2.shape[0]
    in_specs = [pl.BlockSpec((PER * rows, hh), lambda j, i: (call, 0))]
    in_specs += [pl.BlockSpec(v.shape, lambda j, i: (0, 0)) for v in g_oth]
    in_specs += [pl.BlockSpec((bn, 2 * hh), lambda j, i: (j, 0)), ANY, ANY]
    args = [g_own, *g_oth, w2, d, after if buf is None else buf]
    return pl.pallas_call(
        make_du_body(call * PER * rows, len(g_oth)),
        grid=(f // bn, PER),
        in_specs=in_specs,
        out_specs=pl.BlockSpec((rows, bn), lambda j, i: (call * PER + i, j)),
        scratch_shapes=[pltpu.VMEM((PER * rows, 2 * hh), BF16), pltpu.VMEM((NSLOT, rows, bn), F32),
                        pltpu.VMEM((SUB, SUB), F32), pltpu.VMEM((SUB, SUB), F32), pltpu.SemaphoreType.DMA((NSLOT,))],
        out_shape=jax.ShapeDtypeStruct((tokens, f), BF16),
        input_output_aliases={} if buf is None else {len(args) - 1: 0},
        compiler_params=params(),
        cost_estimate=cost(2 * PER * rows * 2 * hh * f, PER * rows * f * 6 + 2 * hh * f * 2),
        name="du",
    )(*args)


def y_body(a_ref, w_ref, *rest):
    rest[-1][...] = dot(a_ref[...], w_ref[...]).astype(BF16)


def dx_body(u_ref, w_ref, *rest):
    rest[-1][...] = dot_t(w_ref[...], u_ref[...]).astype(BF16).T


def out_kernel(body, name, a, w, w_shape, hh, first, count, buf, after, bm=512):
    tokens, f = a.shape
    if name == "y":
        bm, first, count = bm // 2, 2 * first, 2 * count
    extra = [v for v in (buf, after) if v is not None]
    return pl.pallas_call(
        body,
        grid=(count,),
        in_specs=[pl.BlockSpec((bm, f), lambda i: (first + i, 0)), pl.BlockSpec(w_shape, lambda i: (0, 0))] + [ANY] * len(extra),
        out_specs=pl.BlockSpec((bm, hh), lambda i: (first + i, 0)),
        out_shape=jax.ShapeDtypeStruct((tokens, hh), BF16),
        input_output_aliases={} if buf is None else {2: 0},
        compiler_params=params(),
        cost_estimate=cost(2 * count * bm * f * hh, count * bm * f * 2 + f * hh * 2),
    )(a, w, *extra)


TR = 512


def transpose_into(t_ref, x_ref):
    for i in range(x_ref.shape[0] // TR):
        sl = pl.ds(i * TR, TR)
        t_ref[:, sl] = x_ref[sl, :].T


def dw2_body(s_ref, g_ref, a_ref, dep_ref, mine_ref, theirs_ref, t_ref, o_ref, sem):
    j, n = pl.program_id(0), pl.num_programs(0)
    m = o_ref.shape[2]

    @pl.when(j == 0)
    def _():
        transpose_into(t_ref, g_ref)

    def copy(step, u, to_ref):
        slot = lax.rem(step, 2)
        cols = lax.rem(2 * step + u, n) * m
        return pltpu.make_async_copy(o_ref.at[2 * slot + u], to_ref.at[:, pl.ds(pl.multiple_of(cols, m), m)], sem.at[slot, u])

    @pl.when(j >= 2)
    def _():
        for u in range(2):
            copy(j - 2, u, mine_ref).wait()

    slot = lax.rem(j, 2)
    r = dot(t_ref[...], a_ref[...])
    o_ref[2 * slot] = r[:, :m]
    o_ref[2 * slot + 1] = r[:, m:]
    for u in range(2):
        owner = lax.div(2 * j + u, n)

        @pl.when(owner == s_ref[1])
        def _():
            copy(j, u, mine_ref).start()

        @pl.when(owner != s_ref[1])
        def _():
            copy(j, u, theirs_ref).start()

    @pl.when(j == n - 1)
    def _():
        for k in range(2):
            for u in range(2):
                copy(j - k, u, mine_ref).wait()


def dw2_kernel(idx, g, a, width, after, bn=512):
    tokens, n = g.shape
    steps = width // bn
    shape = jax.ShapeDtypeStruct((n, width // 2), F32)
    return pl.pallas_call(
        dw2_body,
        grid_spec=pltpu.PrefetchScalarGridSpec(
            num_scalar_prefetch=1,
            grid=(steps,),
            in_specs=[
                pl.BlockSpec((tokens, n), lambda j, s: (0, 0)),
                pl.BlockSpec((tokens, bn), lambda j, s: (0, s[0] * steps + j)),
                ANY,
            ],
            out_specs=[ANY, ANY],
            scratch_shapes=[pltpu.VMEM((n, tokens), BF16), pltpu.VMEM((4, n, bn // 2), F32), pltpu.SemaphoreType.DMA((2, 2))]),
        out_shape=[shape, shape],
        compiler_params=params(),
        cost_estimate=cost(2 * tokens * n * width, tokens * (n + width) * 2 + n * width * 4),
        name="dw2",
    )(idx, g, a, after)


def dw1_body(s_ref, own_ref, *rest):
    *oth_refs, u_ref, dep_ref, mine_ref, theirs_ref, x_ref, t_ref, sem = rest

    @pl.when(pl.program_id(0) == 0)
    def _():
        @pl.when(s_ref[0] == 0)
        def _():
            cp = pltpu.make_async_copy(own_ref, x_ref, sem.at[0])
            cp.start()
            cp.wait()

        @pl.when(s_ref[0] != 0)
        def _():
            cps, at = [], 0
            for i, ref in enumerate(oth_refs):
                cps.append(pltpu.make_async_copy(ref, x_ref.at[pl.ds(at, ref.shape[0]), :], sem.at[i]))
                at += ref.shape[0]
            for cp in cps:
                cp.start()
            for cp in cps:
                cp.wait()

        transpose_into(t_ref, x_ref)

    r = dot(t_ref[...], u_ref[...])
    half = r.shape[0] // 2

    @pl.when(s_ref[2] == 0)
    def _():
        mine_ref[...] = r[:half]
        theirs_ref[...] = r[half:]

    @pl.when(s_ref[2] != 0)
    def _():
        mine_ref[...] = r[half:]
        theirs_ref[...] = r[:half]


def dw1_kernel(s, x_own, x_oth, du, width, after, bn=512):
    tokens, hh = x_own.shape
    steps = width // bn
    out_spec = pl.BlockSpec((hh // 2, bn), lambda j, s: (0, j))
    shape = jax.ShapeDtypeStruct((hh // 2, width), F32)
    return pl.pallas_call(
        dw1_body,
        grid_spec=pltpu.PrefetchScalarGridSpec(
            num_scalar_prefetch=1,
            grid=(steps,),
            in_specs=[ANY] * (1 + len(x_oth)) + [pl.BlockSpec((tokens, bn), lambda j, s: (0, s[1] * steps + j)), ANY],
            out_specs=[out_spec, out_spec],
            scratch_shapes=[pltpu.VMEM((tokens, hh), BF16), pltpu.VMEM((hh, tokens), BF16), pltpu.SemaphoreType.DMA((len(x_oth),))]),
        out_shape=[shape, shape],
        compiler_params=params(),
        cost_estimate=cost(2 * tokens * hh * width, tokens * (hh + width) * 2 + hh * width * 4),
        name="dw1",
    )(s, x_own, *x_oth, du, after)


def sum_body(here_ref, got_ref, came_ref, o_ref):
    o_ref[...] = (here_ref[...] + got_ref[...]) + came_ref[...]


def sum_kernel(here, got, came, at, steps):
    n, m = came.shape
    bm = n // steps
    plain = pl.BlockSpec((bm, m), lambda i: (i, 0))
    return pl.pallas_call(
        sum_body,
        grid=(steps,),
        in_specs=[pl.BlockSpec((bm, m), at), pl.BlockSpec((bm, m), at), plain],
        out_specs=plain,
        out_shape=jax.ShapeDtypeStruct((n, m), F32),
        compiler_params=params(),
        cost_estimate=cost(2 * n * m, 16 * n * m),
        name="layer_sum",
    )(here, got, came)


def fin2_body(*refs):
    *ins, o_ref = refs
    at = 0
    for a_ref, b_ref in zip(ins[::2], ins[1::2]):
        n = a_ref.shape[0]
        o_ref[:, at:at + n] = (a_ref[...] + b_ref[...]).T
        at += n


def fin2_kernel(pairs, bn=256):
    width = pairs[0][0].shape[1]
    flat = [v for pair in pairs for v in pair]
    n = sum(v.shape[0] for v in flat) // 2
    return pl.pallas_call(
        fin2_body,
        grid=(width // bn,),
        in_specs=[pl.BlockSpec((v.shape[0], bn), lambda j: (0, j)) for v in flat],
        out_specs=pl.BlockSpec((bn, n), lambda j: (j, 0)),
        out_shape=jax.ShapeDtypeStruct((width, n), F32),
        compiler_params=params(),
        cost_estimate=cost(n * width, 12 * n * width),
        name="fin2",
    )(*flat)


def solution(mesh):
    nx = mesh.shape["row"] // 2
    act_spec = P(("depth", "row"), "col")
    weight_spec = P("row", "col")
    pair = [(0, 1), (1, 0)]
    core_pair = [(r, r ^ 1) for r in range(2 * nx)]
    x_pair = [(r, r ^ 2) for r in range(2 * nx)]

    def over_core(v):
        return lax.ppermute(v, "row", core_pair)

    def over_x(v):
        return lax.ppermute(v, "row", x_pair)

    def over_col(v):
        return lax.ppermute(v, "col", pair)

    def over_depth(v):
        return lax.ppermute(v, "depth", pair)

    def body(tok, up, down, grad):
        col = lax.axis_index("col")
        row = lax.axis_index("row")
        x, core = row // 2, row % 2
        tokens, hh = tok.shape
        rows = tokens // NHALF
        fh = up.shape[1]

        w1, w2, tok_first, *cut = gather_kernel(up, down, tok, grad, rows)
        tok_later = over_col(cut[0])
        grad_oth = [over_col(cut[1 + i]) for i in range(NHALF)]

        outs = {"y": None, "dx": None}
        parts = {"y": ((0, 4), (4, 2), (6, 2)), "dx": ((0, 4), (4, 4))}

        def out_part(key, part, after=None):
            args = (y_body, "y", a, w2, (w2.shape[0], hh)) if key == "y" else (dx_body, "dx", du, w1, (hh, w1.shape[1]))
            outs[key] = out_kernel(*args, hh, *parts[key][part], outs[key], after)
            return outs[key]

        a, d = up_kernel(tok, (tok_first,), w1, 0, None, None)
        dep = out_part("y", 0, w1)
        a, d = up_kernel(tok, (tok_later,), w1, 1, (a, d), dep)

        away = dw2_kernel(jnp.stack([1 - x, core]), grad, a, fh, d)
        here = dw2_kernel(jnp.stack([x, core]), grad, a, fh, away[0])
        got_away = over_core(away[1])
        got_here = over_core(here[1])
        pieces, at = [], 0
        for n in (256, hh - 256):
            came = over_x(away[0][at:at + n] + got_away[at:at + n])
            layer = sum_kernel(here[0], got_here, came, lambda i, at=at: (at // 128 + i, 0), n // 128)
            pieces.append((layer, over_depth(layer)))
            at += n
        dw_down = fin2_kernel(pieces)

        du = None
        for i in range(NHALF):
            du = du_kernel(grad, (grad_oth[i],), w2, d, rows // PER, i, du, here[0])

        away = dw1_kernel(jnp.stack([(1 - x + col) % 2, col, core]), tok, (tok_first, tok_later), du, fh, du)
        here = dw1_kernel(jnp.stack([(x + col) % 2, col, core]), tok, (tok_first, tok_later), du, fh, away[0])
        got_away = over_core(away[1])
        got_here = over_core(here[1])
        cols = []
        w = fh // NPIECE1
        for p in range(NPIECE1):
            sl = slice(p * w, (p + 1) * w)
            out = away[0][:, sl] + got_away[:, sl]
            came = over_x(out)
            layer = sum_kernel(here[0], got_here, came, lambda i, p=p: (i, p), 2)
            cols.append(layer + over_depth(layer))
        dw_up = jnp.concatenate(cols, axis=1)

        out_part("y", 1, here[0])
        out_part("y", 2)
        out_part("dx", 0, outs["y"])
        out_part("dx", 1)
        return outs["y"], outs["dx"], dw_up, dw_down

    return jax.shard_map(body, mesh=mesh, in_specs=(act_spec, weight_spec, weight_spec, act_spec),
                         out_specs=(act_spec, act_spec, weight_spec, weight_spec), check_vma=False)
```

```python
import jax
import jax.numpy as jnp
from jax import lax
from jax.experimental import pallas as pl
from jax.experimental.pallas import tpu as pltpu
from jax.sharding import PartitionSpec as P


BF16, F32 = jnp.bfloat16, jnp.float32
VMEM_LIMIT = 60 * 1024 * 1024
SQRT_2_OVER_PI = 0.7978845608028654
CUBIC = 0.044715
NHALF = 2
WIDTHS = (1024, 1024, 512)
PER = 2
NSLOT = 3
PIECE = 128
TILE = 16
SUB = 512
MESH = pl.DeviceIdType.MESH
LAST_LAST = (((1,), (1,)), ((), ()))


def dot(a, b):
    return jnp.dot(a, b, preferred_element_type=F32)


def dot_t(a, b):
    return lax.dot_general(a, b, LAST_LAST, preferred_element_type=F32)


def cost(flops, nbytes, trans=0):
    return pl.CostEstimate(flops=flops, bytes_accessed=nbytes, transcendentals=trans)


def params():
    return pltpu.CompilerParams(vmem_limit_bytes=VMEM_LIMIT)


def gather_body(w1_ref, w2_ref, tok_ref, grad_ref, w1, w2, tok_oth, *rest):
    *cut, v1, v2, vt, vg, send, recv, load, store = rest
    col, row, depth = lax.axis_index("col"), lax.axis_index("row"), lax.axis_index("depth")
    x, core = row // 2, row % 2
    to_core = {"row": 2 * x + (1 - core)}
    to_x = {"row": 2 * (1 - x) + core}
    to_col = {"col": 1 - col}
    to_depth = {"depth": 1 - depth}

    barrier = pltpu.get_barrier_semaphore()
    for dev in (to_core, to_x, to_col, to_depth):
        pl.semaphore_signal(barrier, inc=1, device_id=dev, device_id_type=MESH)
    pl.semaphore_wait(barrier, 4)

    def place(which, bx, bcol, at_col, half=None):
        ref = (w1_ref, w2_ref)[which]
        n, m = ref.shape
        side = (bx + at_col) % 2 if which == 0 else (bcol + at_col) % 2
        if which == 0:
            r0, c0 = side * (2 * n) + core * n, bcol * m
        else:
            r0, c0 = (2 * bx + core) * n, side * m
        if half is not None:
            r0, n = r0 + half * (n // 2), n // 2
        return (w1, w2)[which].at[pl.ds(pl.multiple_of(r0, 32), n), pl.ds(pl.multiple_of(c0, 128), m)]

    made = []

    def start(src, dst, dev):
        i = len(made)
        cp = pltpu.make_async_remote_copy(src_ref=src, dst_ref=dst, send_sem=send.at[i], recv_sem=recv.at[i],
                                          device_id=dev, device_id_type=MESH)
        cp.start()
        made.append(cp)
        return cp

    def forward(piece, dev):
        return start(piece, piece, dev)

    def half_of(ref):
        n = ref.shape[0] // 2
        return ref.at[pl.ds(pl.multiple_of(depth * n, 32), n), :]

    late = []

    def to_partner(piece):
        late.append(forward(piece, to_core))

    other = 1 - col
    col1 = start(half_of(w1_ref), place(0, x, col, other, depth), to_col)
    x1 = start(w1_ref, place(0, x, col, col), to_x)
    col2 = start(half_of(w2_ref), place(1, x, col, other, depth), to_col)
    first = tok_oth.shape[0]
    late.append(start(tok_ref.at[pl.ds(0, first), :], tok_oth, to_col))
    late.append(start(w1_ref, place(0, x, col, col), to_core))
    late.append(start(w2_ref, place(1, x, col, col), to_core))
    size = tok_oth.shape[0]
    loads = [pltpu.make_async_copy(w1_ref, v1, load.at[0]), pltpu.make_async_copy(w2_ref, v2, load.at[1]),
             pltpu.make_async_copy(tok_ref.at[pl.ds(size, size), :], vt, load.at[2]),
             pltpu.make_async_copy(grad_ref, vg, load.at[3])]
    for cp in loads:
        cp.start()
    for cp in loads:
        cp.wait()
    keep = [pltpu.make_async_copy(v1, place(0, x, col, col), store.at[0]),
            pltpu.make_async_copy(v2, place(1, x, col, col), store.at[1])]
    spans = [(vt, 0)] + [(vg, i) for i in range(NHALF)]
    for j, (src, i) in enumerate(spans):
        keep.append(pltpu.make_async_copy(src.at[pl.ds(i * size, size), :], cut[j], store.at[2 + j]))
    for cp in keep:
        cp.start()

    def oth(which, bx, half):
        return place(which, bx, other, col, half)

    col1.wait_recv()
    z1 = forward(oth(0, x, depth), to_depth)
    x1h = forward(oth(0, x, depth), to_x)
    to_partner(oth(0, x, depth))
    x2 = start(half_of(w2_ref), place(1, x, col, col, depth), to_x)
    col2.wait_recv()
    z2 = forward(oth(1, x, depth), to_depth)
    x2h = forward(oth(1, x, depth), to_x)
    to_partner(oth(1, x, depth))
    z1.wait_recv()
    to_partner(oth(0, x, 1 - depth))
    x1.wait_recv()
    to_partner(place(0, 1 - x, col, col))
    x1h.wait_recv()
    z1d = forward(oth(0, 1 - x, depth), to_depth)
    to_partner(oth(0, 1 - x, depth))
    z2.wait_recv()
    to_partner(oth(1, x, 1 - depth))
    x2.wait_recv()
    z2o = forward(place(1, 1 - x, col, col, depth), to_depth)
    to_partner(place(1, 1 - x, col, col, depth))
    z1d.wait_recv()
    to_partner(oth(0, 1 - x, 1 - depth))
    x2h.wait_recv()
    z2d = forward(oth(1, 1 - x, depth), to_depth)
    to_partner(oth(1, 1 - x, depth))
    z2o.wait_recv()
    to_partner(place(1, 1 - x, col, col, 1 - depth))
    z2d.wait_recv()
    to_partner(oth(1, 1 - x, 1 - depth))
    for cp in late:
        cp.wait_recv()
    for cp in made:
        cp.wait_send()
    for cp in keep:
        cp.wait()


NCOPY = 25
NCUT = 1 + NHALF


def gather_kernel(up, down, tok, grad, rows):
    piece = jax.ShapeDtypeStruct((rows, tok.shape[1]), BF16)
    return pl.pallas_call(
        gather_body,
        in_specs=[pl.BlockSpec(memory_space=pl.ANY)] * 4,
        out_specs=[pl.BlockSpec(memory_space=pl.ANY)] * (3 + NCUT),
        out_shape=[jax.ShapeDtypeStruct((4 * up.shape[0], 2 * up.shape[1]), BF16),
                   jax.ShapeDtypeStruct((4 * down.shape[0], 2 * down.shape[1]), BF16),
                   piece] + [piece] * NCUT,
        scratch_shapes=[pltpu.VMEM(up.shape, BF16), pltpu.VMEM(down.shape, BF16),
                        pltpu.VMEM((rows, tok.shape[1]), BF16), pltpu.VMEM(grad.shape, BF16),
                        pltpu.SemaphoreType.DMA((NCOPY,)), pltpu.SemaphoreType.DMA((NCOPY,)),
                        pltpu.SemaphoreType.DMA((4,)), pltpu.SemaphoreType.DMA((2 + NCUT,))],
        compiler_params=pltpu.CompilerParams(collective_id=0, has_side_effects=True, vmem_limit_bytes=VMEM_LIMIT),
        cost_estimate=cost(0, 300_000_000),
        name="gather",
    )(up, down, tok, grad)


ANY = pl.BlockSpec(memory_space=pl.ANY)


def make_up_body(first_row, nlater, per):
    def up_body(xo_ref, *rest):
        xt_refs, w_ref = rest[:nlater], rest[nlater]
        a_hbm, d_hbm, x_ref, u0_ref, u1_ref, a_ref, d_ref, sem = rest[-8:]
        rows, hh = a_ref.shape[1], xo_ref.shape[1]
        piece = u0_ref.shape[0]
        last = rows // piece - 1
        bn = w_ref.shape[1]
        j, n = pl.program_id(0) * per + pl.program_id(1), pl.num_programs(0) * per
        row = pl.multiple_of(pl.program_id(1) * rows, rows)

        def copies(step, part):
            slot = lax.rem(step, NSLOT)
            cols = pl.ds(pl.multiple_of(lax.div(step, per) * bn, bn), bn)
            base = pl.multiple_of(first_row + lax.rem(step, per) * rows, rows)
            first, size = ((0, last * piece), (last * piece, piece))[part]
            src, dst = pl.ds(first, size), pl.ds(base + first, size)
            return (pltpu.make_async_copy(a_ref.at[slot, src], a_hbm.at[dst, cols], sem.at[0, part, slot]),
                    pltpu.make_async_copy(d_ref.at[slot, src], d_hbm.at[dst, cols], sem.at[1, part, slot]))

        def start(step, part):
            for cp in copies(step, part):
                cp.start()

        def wait(step, part):
            for cp in copies(step, part):
                cp.wait()

        def finish(u_ref, slot, which):
            for r in range(0, piece, TILE):
                u = u_ref[pl.ds(r, TILE), :]
                sl = pl.ds(which * piece + r, TILE)
                u2 = u * u
                t = jnp.tanh(u * (SQRT_2_OVER_PI + (SQRT_2_OVER_PI * CUBIC) * u2))
                h = 0.5 + 0.5 * t
                act = u * h
                a_ref[slot, sl, :] = act.astype(BF16)
                slope = 2.0 * SQRT_2_OVER_PI + (6.0 * SQRT_2_OVER_PI * CUBIC) * u2
                d_ref[slot, sl, :] = h + (h * (u - act)) * slope

        @pl.when(j == 0)
        def _():
            x_ref[:, :hh] = xo_ref[...]
            at = 0
            for ref in xt_refs:
                x_ref[at:at + ref.shape[0], hh:] = ref[...]
                at += ref.shape[0]

        @pl.when(j >= NSLOT)
        def _():
            wait(j - NSLOT, 0)

        @pl.when(j >= NSLOT + 1)
        def _():
            wait(j - NSLOT - 1, 1)

        slot, prev = lax.rem(j, NSLOT), lax.rem(j + NSLOT - 1, NSLOT)
        held = (u0_ref, u1_ref)
        for i in range(last + 1):
            held[i % 2][...] = dot(x_ref[pl.ds(row + i * piece, piece), :], w_ref[...])
            if i == 0:
                finish(held[last % 2], prev, last)
            else:
                finish(held[(i - 1) % 2], slot, i - 1)
        start(j, 0)

        @pl.when(j >= 1)
        def _():
            start(j - 1, 1)

        @pl.when(j == n - 1)
        def _():
            wait(j - NSLOT, 1)
            finish(held[last % 2], slot, last)
            start(j, 1)
            for k in range(NSLOT):
                wait(j - k, 0)
                wait(j - k, 1)

    return up_body


def up_kernel(x_own, x_oth, w1, call, bufs, after, rows=1024, bn=512):
    tokens, hh = x_own.shape
    f = w1.shape[1]
    total = sum(v.shape[0] for v in x_oth)
    in_specs = [pl.BlockSpec((total, hh), lambda j, i: (call, 0))]
    in_specs += [pl.BlockSpec(v.shape, lambda j, i: (0, 0)) for v in x_oth]
    in_specs += [pl.BlockSpec((2 * hh, bn), lambda j, i: (0, j))]
    args = [x_own, *x_oth, w1]
    aliases = {}
    if bufs is not None:
        aliases = {len(args): 0, len(args) + 1: 1}
        in_specs += [ANY] * 3
        args += [*bufs, after]
    return pl.pallas_call(
        make_up_body(call * total, len(x_oth), total // rows),
        grid=(f // bn, total // rows),
        in_specs=in_specs,
        out_specs=[ANY, ANY],
        scratch_shapes=[pltpu.VMEM((total, 2 * hh), BF16), pltpu.VMEM((PIECE, bn), F32), pltpu.VMEM((PIECE, bn), F32),
                        pltpu.VMEM((NSLOT, rows, bn), BF16), pltpu.VMEM((NSLOT, rows, bn), F32), pltpu.SemaphoreType.DMA((2, 2, NSLOT))],
        out_shape=[jax.ShapeDtypeStruct((tokens, f), BF16), jax.ShapeDtypeStruct((tokens, f), F32)],
        input_output_aliases=aliases,
        compiler_params=params(),
        cost_estimate=cost(2 * total * 2 * hh * f, total * f * 6 + 2 * hh * f * 2, total * f),
        name="up",
    )(*args)


def make_du_body(first_row, nlater):
    def du_body(go_ref, *rest):
        gt_refs, w_ref, d_hbm = rest[:nlater], rest[nlater], rest[nlater + 1]
        u_ref, g_ref, d_ref, a0_ref, a1_ref, sem = rest[-6:]
        rows, hh = u_ref.shape[0], go_ref.shape[1]
        bn = w_ref.shape[0]
        j, n = pl.program_id(0) * PER + pl.program_id(1), pl.num_programs(0) * PER
        row = pl.multiple_of(pl.program_id(1) * rows, rows)

        def copy(step):
            slot = lax.rem(step, NSLOT)
            cols = pl.ds(pl.multiple_of(lax.div(step, PER) * bn, bn), bn)
            base = pl.multiple_of(first_row + lax.rem(step, PER) * rows, rows)
            return pltpu.make_async_copy(d_hbm.at[pl.ds(base, rows), cols], d_ref.at[slot], sem.at[slot])

        @pl.when(j == 0)
        def _():
            for k in range(NSLOT - 1):
                copy(k).start()
            g_ref[:, :hh] = go_ref[...]
            at = 0
            for ref in gt_refs:
                g_ref[at:at + ref.shape[0], hh:] = ref[...]
                at += ref.shape[0]

        @pl.when(j + NSLOT - 1 < n)
        def _():
            copy(j + NSLOT - 1).start()

        copy(j).wait()
        slot = lax.rem(j, NSLOT)
        held = (a0_ref, a1_ref)
        blocks = [(i, k) for k in range(bn // SUB) for i in range(rows // SUB)]

        def finish(ref, i, k):
            for r in range(0, SUB, TILE):
                sl, sk = pl.ds(i * SUB + r, TILE), pl.ds(k * SUB, SUB)
                u_ref[sl, sk] = (ref[pl.ds(r, TILE), :] * d_ref[slot, sl, sk]).astype(BF16)

        for m, (i, k) in enumerate(blocks):
            held[m % 2][...] = dot_t(g_ref[pl.ds(row + i * SUB, SUB), :], w_ref[pl.ds(k * SUB, SUB), :])
            if m:
                finish(held[(m - 1) % 2], *blocks[m - 1])
        finish(held[(len(blocks) - 1) % 2], *blocks[-1])

    return du_body


def du_kernel(g_own, g_oth, w2, d, rows, call, buf, after, bn=1024):
    tokens, hh = g_own.shape
    f = w2.shape[0]
    in_specs = [pl.BlockSpec((PER * rows, hh), lambda j, i: (call, 0))]
    in_specs += [pl.BlockSpec(v.shape, lambda j, i: (0, 0)) for v in g_oth]
    in_specs += [pl.BlockSpec((bn, 2 * hh), lambda j, i: (j, 0)), ANY, ANY]
    args = [g_own, *g_oth, w2, d, after if buf is None else buf]
    return pl.pallas_call(
        make_du_body(call * PER * rows, len(g_oth)),
        grid=(f // bn, PER),
        in_specs=in_specs,
        out_specs=pl.BlockSpec((rows, bn), lambda j, i: (call * PER + i, j)),
        scratch_shapes=[pltpu.VMEM((PER * rows, 2 * hh), BF16), pltpu.VMEM((NSLOT, rows, bn), F32),
                        pltpu.VMEM((SUB, SUB), F32), pltpu.VMEM((SUB, SUB), F32), pltpu.SemaphoreType.DMA((NSLOT,))],
        out_shape=jax.ShapeDtypeStruct((tokens, f), BF16),
        input_output_aliases={} if buf is None else {len(args) - 1: 0},
        compiler_params=params(),
        cost_estimate=cost(2 * PER * rows * 2 * hh * f, PER * rows * f * 6 + 2 * hh * f * 2),
        name="du",
    )(*args)


def y_body(a_ref, w_ref, *rest):
    rest[-1][...] = dot(a_ref[...], w_ref[...]).astype(BF16)


def dx_body(u_ref, w_ref, *rest):
    rest[-1][...] = dot_t(w_ref[...], u_ref[...]).astype(BF16).T


def out_kernel(body, name, a, w, w_shape, hh, first, count, buf, after, bm=512):
    tokens, f = a.shape
    if name == "y":
        bm, first, count = bm // 2, 2 * first, 2 * count
    extra = [v for v in (buf, after) if v is not None]
    return pl.pallas_call(
        body,
        grid=(count,),
        in_specs=[pl.BlockSpec((bm, f), lambda i: (first + i, 0)), pl.BlockSpec(w_shape, lambda i: (0, 0))] + [ANY] * len(extra),
        out_specs=pl.BlockSpec((bm, hh), lambda i: (first + i, 0)),
        out_shape=jax.ShapeDtypeStruct((tokens, hh), BF16),
        input_output_aliases={} if buf is None else {2: 0},
        compiler_params=params(),
        cost_estimate=cost(2 * count * bm * f * hh, count * bm * f * 2 + f * hh * 2),
    )(a, w, *extra)


TR = 512


def transpose_into(t_ref, x_ref):
    for i in range(x_ref.shape[0] // TR):
        sl = pl.ds(i * TR, TR)
        t_ref[:, sl] = x_ref[sl, :].T


def dw2_body(s_ref, g_ref, a_ref, dep_ref, mine_ref, theirs_ref, t_ref, o_ref, sem):
    j, n = pl.program_id(0), pl.num_programs(0)
    m = o_ref.shape[2]

    @pl.when(j == 0)
    def _():
        transpose_into(t_ref, g_ref)

    def copy(step, u, to_ref):
        slot = lax.rem(step, 2)
        cols = lax.rem(2 * step + u, n) * m
        return pltpu.make_async_copy(o_ref.at[2 * slot + u], to_ref.at[:, pl.ds(pl.multiple_of(cols, m), m)], sem.at[slot, u])

    @pl.when(j >= 2)
    def _():
        for u in range(2):
            copy(j - 2, u, mine_ref).wait()

    slot = lax.rem(j, 2)
    r = dot(t_ref[...], a_ref[...])
    o_ref[2 * slot] = r[:, :m]
    o_ref[2 * slot + 1] = r[:, m:]
    for u in range(2):
        owner = lax.div(2 * j + u, n)

        @pl.when(owner == s_ref[1])
        def _():
            copy(j, u, mine_ref).start()

        @pl.when(owner != s_ref[1])
        def _():
            copy(j, u, theirs_ref).start()

    @pl.when(j == n - 1)
    def _():
        for k in range(2):
            for u in range(2):
                copy(j - k, u, mine_ref).wait()


def dw2_kernel(idx, g, a, width, after, bn=512):
    tokens, n = g.shape
    steps = width // bn
    shape = jax.ShapeDtypeStruct((n, width // 2), F32)
    return pl.pallas_call(
        dw2_body,
        grid_spec=pltpu.PrefetchScalarGridSpec(
            num_scalar_prefetch=1,
            grid=(steps,),
            in_specs=[
                pl.BlockSpec((tokens, n), lambda j, s: (0, 0)),
                pl.BlockSpec((tokens, bn), lambda j, s: (0, s[0] * steps + j)),
                ANY,
            ],
            out_specs=[ANY, ANY],
            scratch_shapes=[pltpu.VMEM((n, tokens), BF16), pltpu.VMEM((4, n, bn // 2), F32), pltpu.SemaphoreType.DMA((2, 2))]),
        out_shape=[shape, shape],
        compiler_params=params(),
        cost_estimate=cost(2 * tokens * n * width, tokens * (n + width) * 2 + n * width * 4),
        name="dw2",
    )(idx, g, a, after)


def dw1_body(s_ref, own_ref, *rest):
    *oth_refs, u_ref, dep_ref, mine_ref, theirs_ref, x_ref, t_ref, sem = rest

    @pl.when(pl.program_id(0) == 0)
    def _():
        @pl.when(s_ref[0] == 0)
        def _():
            cp = pltpu.make_async_copy(own_ref, x_ref, sem.at[0])
            cp.start()
            cp.wait()

        @pl.when(s_ref[0] != 0)
        def _():
            cps, at = [], 0
            for i, ref in enumerate(oth_refs):
                cps.append(pltpu.make_async_copy(ref, x_ref.at[pl.ds(at, ref.shape[0]), :], sem.at[i]))
                at += ref.shape[0]
            for cp in cps:
                cp.start()
            for cp in cps:
                cp.wait()

        transpose_into(t_ref, x_ref)

    r = dot(t_ref[...], u_ref[...])
    half = r.shape[0] // 2

    @pl.when(s_ref[2] == 0)
    def _():
        mine_ref[...] = r[:half]
        theirs_ref[...] = r[half:]

    @pl.when(s_ref[2] != 0)
    def _():
        mine_ref[...] = r[half:]
        theirs_ref[...] = r[:half]


def dw1_kernel(s, x_own, x_oth, du, width, after, bn=512):
    tokens, hh = x_own.shape
    steps = width // bn
    out_spec = pl.BlockSpec((hh // 2, bn), lambda j, s: (0, j))
    shape = jax.ShapeDtypeStruct((hh // 2, width), F32)
    return pl.pallas_call(
        dw1_body,
        grid_spec=pltpu.PrefetchScalarGridSpec(
            num_scalar_prefetch=1,
            grid=(steps,),
            in_specs=[ANY] * (1 + len(x_oth)) + [pl.BlockSpec((tokens, bn), lambda j, s: (0, s[1] * steps + j)), ANY],
            out_specs=[out_spec, out_spec],
            scratch_shapes=[pltpu.VMEM((tokens, hh), BF16), pltpu.VMEM((hh, tokens), BF16), pltpu.SemaphoreType.DMA((len(x_oth),))]),
        out_shape=[shape, shape],
        compiler_params=params(),
        cost_estimate=cost(2 * tokens * hh * width, tokens * (hh + width) * 2 + hh * width * 4),
        name="dw1",
    )(s, x_own, *x_oth, du, after)


def sum_body(here_ref, got_ref, came_ref, o_ref):
    o_ref[...] = (here_ref[...] + got_ref[...]) + came_ref[...]


def sum_kernel(here, got, came, at, steps):
    n, m = came.shape
    bm = n // steps
    plain = pl.BlockSpec((bm, m), lambda i: (i, 0))
    return pl.pallas_call(
        sum_body,
        grid=(steps,),
        in_specs=[pl.BlockSpec((bm, m), at), pl.BlockSpec((bm, m), at), plain],
        out_specs=plain,
        out_shape=jax.ShapeDtypeStruct((n, m), F32),
        compiler_params=params(),
        cost_estimate=cost(2 * n * m, 16 * n * m),
        name="layer_sum",
    )(here, got, came)


def fin2_body(*refs):
    *ins, o_ref = refs
    at = 0
    for a_ref, b_ref in zip(ins[::2], ins[1::2]):
        n = a_ref.shape[0]
        o_ref[:, at:at + n] = (a_ref[...] + b_ref[...]).T
        at += n


def fin2_kernel(pairs, bn=256):
    width = pairs[0][0].shape[1]
    flat = [v for pair in pairs for v in pair]
    n = sum(v.shape[0] for v in flat) // 2
    return pl.pallas_call(
        fin2_body,
        grid=(width // bn,),
        in_specs=[pl.BlockSpec((v.shape[0], bn), lambda j: (0, j)) for v in flat],
        out_specs=pl.BlockSpec((bn, n), lambda j: (j, 0)),
        out_shape=jax.ShapeDtypeStruct((width, n), F32),
        compiler_params=params(),
        cost_estimate=cost(n * width, 12 * n * width),
        name="fin2",
    )(*flat)


def solution(mesh):
    nx = mesh.shape["row"] // 2
    act_spec = P(("depth", "row"), "col")
    weight_spec = P("row", "col")
    pair = [(0, 1), (1, 0)]
    core_pair = [(r, r ^ 1) for r in range(2 * nx)]
    x_pair = [(r, r ^ 2) for r in range(2 * nx)]

    def over_core(v):
        return lax.ppermute(v, "row", core_pair)

    def over_x(v):
        return lax.ppermute(v, "row", x_pair)

    def over_col(v):
        return lax.ppermute(v, "col", pair)

    def over_depth(v):
        return lax.ppermute(v, "depth", pair)

    def body(tok, up, down, grad):
        col = lax.axis_index("col")
        row = lax.axis_index("row")
        x, core = row // 2, row % 2
        tokens, hh = tok.shape
        rows = tokens // NHALF
        fh = up.shape[1]

        w1, w2, tok_first, *cut = gather_kernel(up, down, tok, grad, rows)
        tok_later = over_col(cut[0])
        grad_oth = [over_col(cut[1 + i]) for i in range(NHALF)]

        outs = {"y": None, "dx": None}
        parts = {"y": ((0, 4), (4, 2), (6, 2)), "dx": ((0, 4), (4, 4))}

        def out_part(key, part, after=None):
            args = (y_body, "y", a, w2, (w2.shape[0], hh)) if key == "y" else (dx_body, "dx", du, w1, (hh, w1.shape[1]))
            outs[key] = out_kernel(*args, hh, *parts[key][part], outs[key], after)
            return outs[key]

        a, d = up_kernel(tok, (tok_first,), w1, 0, None, None)
        dep = out_part("y", 0, w1)
        a, d = up_kernel(tok, (tok_later,), w1, 1, (a, d), dep)

        away = dw2_kernel(jnp.stack([1 - x, core]), grad, a, fh, d)
        here = dw2_kernel(jnp.stack([x, core]), grad, a, fh, away[0])
        got_away = over_core(away[1])
        got_here = over_core(here[1])
        pieces, at = [], 0
        for n in (256, hh - 256):
            came = over_x(away[0][at:at + n] + got_away[at:at + n])
            layer = sum_kernel(here[0], got_here, came, lambda i, at=at: (at // 128 + i, 0), n // 128)
            pieces.append((layer, over_depth(layer)))
            at += n
        dw_down = fin2_kernel(pieces)

        du = None
        for i in range(NHALF):
            du = du_kernel(grad, (grad_oth[i],), w2, d, rows // PER, i, du, here[0])

        away = dw1_kernel(jnp.stack([(1 - x + col) % 2, col, core]), tok, (tok_first, tok_later), du, fh, du)
        here = dw1_kernel(jnp.stack([(x + col) % 2, col, core]), tok, (tok_first, tok_later), du, fh, away[0])
        got_away = over_core(away[1])
        got_here = over_core(here[1])
        cols = []
        at = 0
        for w in WIDTHS:
            sl = slice(at, at + w)
            came = over_x(away[0][:, sl] + got_away[:, sl])
            layer = sum_kernel(here[0], got_here, came, lambda i, q=at // w: (i, q), 2)
            cols.append(layer + over_depth(layer))
            at += w
        dw_up = jnp.concatenate(cols, axis=1)

        out_part("y", 1, here[0])
        out_part("y", 2)
        out_part("dx", 0, outs["y"])
        out_part("dx", 1)
        return outs["y"], outs["dx"], dw_up, dw_down

    return jax.shard_map(body, mesh=mesh, in_specs=(act_spec, weight_spec, weight_spec, act_spec),
                         out_specs=(act_spec, act_spec, weight_spec, weight_spec), check_vma=False)
```
